256 devices in a mesh: gx: 2 (over core), gy: 2 (over x_lo), gz: 64 (over z, y, x_hi).
Axes of the slice: x: 4 (x_hi: 2, x_lo: 2; x = x_hi * 2 + x_lo), y: 4, z: 8, core: 2. Of those that a mesh axis runs over, the one named last changes fastest.
Arguments:
- old_pos: float32 [3, 262144], P(None, ('gx', 'gy', 'gz')), may hold values from -6 to 6
- new_pos: float32 [3, 262144], P(None, ('gx', 'gy', 'gz')), may hold values from -6 to 6
- inv_mass: float32 [262144], P(('gx', 'gy', 'gz')), may hold values from 0.05 to 1
- rest_length: float32 [262144], P(('gx', 'gy', 'gz')), may hold values from 0.8 to 1.6
- bond_pairs: int32 [2, 262144], P(None, ('gx', 'gy', 'gz')), may hold values from 0 to 1311, as said below
- live: int32 [262144], P(('gx', 'gy', 'gz')), may hold values from 0 to 1, as said below
- send_index: int32 [1536, 48], P(('gx', 'gy', 'gz')), may hold values from 0 to 1023, as said below
Outputs:
- displacement: float32 [3, 262144], P(None, ('gx', 'gy', 'gz'))
- multipliers: float32 [262144], P(('gx', 'gy', 'gz'))
The draws below stay inside these ranges and needn't reach their ends.
Inputs may be any that keep to these rules, and one draw needn't show every extreme that they name: `bond_pairs`: in domain k's slots, row 0 is an own atom (0 to 1023). Row 1 indexes the domain's extended list: its own atoms, then six blocks of 48 received atoms, block 2a + s holding, in order, list 2a + s of the neighbour one step down (s = 0) or up (s = 1) along axis a. Every atom is in at most two live constraints, each received atom is the second atom of at most one live constraint, and exactly 216 live constraints of each domain name a received atom. `live`: padding slots change nothing. `send_index`: rows 6k to 6k + 5 are domain k's lists of own atoms; list 2a + s goes to the neighbour one step up (s = 0) or down (s = 1) along axis a, periodically. The 288 entries of a domain are distinct.
All inputs are finite; a program needn't handle non-finite values.
Results may differ from the reference program's by a relative error of at most 0.0001.
Values sent between devices are 32-bit elements; how exact they have to be, the bound alone decides.
A program may use at most 64 MiB of HBM per device.

```python
import math
import jax
import jax.numpy as jnp
from jax import lax

ATOMS_DEV = 1024
HALO_ROWS = 48
CHAIN_HEADS = 384
CROSS_BONDS = 216
ORDER = 4
DOMAINS = 256
ATOMS = 262144
N_GX = 2
N_GY = 2
N_GZ = 64


def one_domain(key):
    keys = jax.random.split(key, 6)
    position = jnp.arange(ATOMS_DEV, dtype=jnp.int32)
    atom_slot = jax.random.permutation(keys[0], ATOMS_DEV).astype(jnp.int32)
    ranking = jax.random.permutation(keys[1], ATOMS_DEV).astype(jnp.int32)
    heading = (ranking < CHAIN_HEADS) | (position == 0)
    ending = jnp.concatenate([heading[1:], jnp.ones((1,), dtype=bool)])
    tiebreak = jax.random.permutation(keys[2], ATOMS_DEV).astype(jnp.int32)
    end_score = ending.astype(jnp.int32) * (1 << 24) + tiebreak
    unused_end, cross_pos = lax.top_k(end_score, CROSS_BONDS)
    halo_slot = jax.random.permutation(keys[3], 6 * HALO_ROWS).astype(jnp.int32)[:CROSS_BONDS] + ATOMS_DEV
    following = jnp.roll(atom_slot, -1)
    second_atom = jnp.where(ending, 0, following).astype(jnp.int32)
    second_atom = second_atom.at[cross_pos].set(halo_slot)
    alive = jnp.where(ending, 0, 1).astype(jnp.int32).at[cross_pos].set(1)
    ordering = jax.random.permutation(keys[4], ATOMS_DEV).astype(jnp.int32)
    first_atom = atom_slot[ordering]
    second_atom = second_atom[ordering]
    alive = alive[ordering]
    head_tie = jax.random.permutation(keys[5], ATOMS_DEV).astype(jnp.int32)
    head_score = heading.astype(jnp.int32) * (1 << 24) + head_tie
    unused_head, head_pos = lax.top_k(head_score, 6 * HALO_ROWS)
    sending = atom_slot[head_pos].reshape(6, HALO_ROWS)
    return (first_atom, second_atom, alive, sending)


def all_domains(key):
    numbers = jnp.arange(DOMAINS, dtype=jnp.int32)
    domain_keys = jax.vmap(lambda number: jax.random.fold_in(key, number))(numbers)
    return jax.vmap(one_domain)(domain_keys)


def draw_bond_pairs(key, part):
    first_atom, second_atom, alive, sending = all_domains(key)
    return jnp.stack([first_atom.reshape(-1), second_atom.reshape(-1)], 0).astype(jnp.int32)


def draw_live(key, part):
    first_atom, second_atom, alive, sending = all_domains(key)
    return alive.reshape(-1).astype(jnp.int32)


def draw_send_index(key, part):
    first_atom, second_atom, alive, sending = all_domains(key)
    return sending.reshape(DOMAINS * 6, HALO_ROWS).astype(jnp.int32)


def block_levels(stream_key, dims, cuts, low, high):
    def one(dim, parts):
        draws = jax.random.uniform(jax.random.fold_in(jax.random.fold_in(stream_key, 6), dim), (parts,), jnp.float32, low / len(cuts), high / len(cuts))
        return jnp.repeat(jnp.exp(draws), dims[dim] // parts).reshape((-1,) + (1,) * (len(dims) - dim - 1))

    level = one(*cuts[0])
    for cut in cuts[1:]:
        level = level * one(*cut)
    return level


def normal_values(key, dims, scale, most, cuts=(), kind=jnp.bfloat16):
    drawn = scale * jax.random.normal(key, dims, jnp.float32)
    if cuts:
        drawn = drawn * block_levels(key, dims, cuts, -0.22, 0.18)
    return jnp.clip(drawn, -most, most).astype(kind)


def setup_inputs(seed: int = 0) -> dict:
    streams_of = jax.random.split(jax.random.key(seed), 8)
    return {
        "old_pos": normal_values(streams_of[0], (3, ATOMS), 1.0, 6.0, ((1, 256),), jnp.float32),
        "new_pos": normal_values(streams_of[1], (3, ATOMS), 1.0, 6.0, ((1, 256),), jnp.float32),
        "inv_mass": jnp.clip(jnp.exp(math.log(1.0) - 2.9957323 * jax.random.uniform(streams_of[2], (ATOMS,), jnp.float32) ** block_levels(streams_of[2], (ATOMS,), ((0, 256),), -0.2, 0.2)), 0.05, 1.0),
        "rest_length": jnp.clip(0.8 + 0.8 * jax.random.uniform(streams_of[3], (ATOMS,), jnp.float32) ** block_levels(streams_of[3], (ATOMS,), ((0, 256),), -0.2, 0.2), 0.8, 1.6),
        "bond_pairs": draw_bond_pairs(jax.random.fold_in(streams_of[7], 71), 0),
        "live": draw_live(jax.random.fold_in(streams_of[7], 71), 0),
        "send_index": draw_send_index(jax.random.fold_in(streams_of[7], 71), 0),
    }


def owners(bond_pairs, send_index):
    slot_index = jnp.arange(ATOMS, dtype=jnp.int32)
    domain = slot_index // ATOMS_DEV
    first_atom = domain * ATOMS_DEV + bond_pairs[0].astype(jnp.int32)
    local_second = bond_pairs[1].astype(jnp.int32)
    remote = local_second >= ATOMS_DEV
    offset = jnp.maximum(local_second - ATOMS_DEV, 0)
    block = offset // HALO_ROWS
    row_index = offset % HALO_ROWS
    coord_x = domain // (N_GY * N_GZ)
    coord_y = domain // N_GZ % N_GY
    coord_z = domain % N_GZ
    stride = jnp.where(block % 2 == 0, -1, 1)
    axis_pick = block // 2
    source_x = (coord_x + jnp.where(axis_pick == 0, stride, 0)) % N_GX
    source_y = (coord_y + jnp.where(axis_pick == 1, stride, 0)) % N_GY
    source_z = (coord_z + jnp.where(axis_pick == 2, stride, 0)) % N_GZ
    source = (source_x * N_GY + source_y) * N_GZ + source_z
    sent_atom = send_index[source * 6 + block, row_index].astype(jnp.int32)
    second_atom = jnp.where(remote, source * ATOMS_DEV + sent_atom, domain * ATOMS_DEV + local_second)
    return (first_atom, second_atom)

def reference(old_pos, new_pos, inv_mass, rest_length, bond_pairs, live, send_index):
    first_atom, second_atom = owners(bond_pairs, send_index)

    def across_bond(field):
        return field[:, first_atom] - field[:, second_atom]
    old_span = across_bond(old_pos)
    unit_dir = old_span / jnp.sqrt(lax.optimization_barrier(jnp.sum(old_span * old_span, 0)) + 0.25)
    scaling = live.astype(jnp.float32) / jnp.sqrt(inv_mass[first_atom] + inv_mass[second_atom])

    def atom_shift(values):
        contrib = unit_dir * (scaling * values)[None]
        blank = jnp.zeros((3, ATOMS), jnp.float32)
        summed = blank.at[:, first_atom].add(contrib).at[:, second_atom].add(-contrib)
        return inv_mass[None] * summed

    def coupling(values):
        return values - scaling * lax.optimization_barrier(jnp.sum(unit_dir * across_bond(atom_shift(values)), 0))

    def expansion(start):
        series = start
        current = start
        for repeat in range(ORDER):
            current = coupling(current)
            series = series + current
        return series
    right_side = scaling * (lax.optimization_barrier(jnp.sum(unit_dir * across_bond(new_pos), 0)) - rest_length)
    first_sol = expansion(right_side)
    shifted_pos = new_pos - atom_shift(first_sol)
    stretch = across_bond(shifted_pos)
    length_sq = lax.optimization_barrier(jnp.sum(stretch * stretch, 0))
    floor_sq = 0.25 * rest_length * rest_length
    target = jnp.sqrt(jnp.maximum(2.0 * rest_length * rest_length - length_sq, floor_sq))
    second_sol = expansion(scaling * (rest_length - target))
    final_pos = shifted_pos - atom_shift(second_sol)
    return (final_pos - new_pos, first_sol + second_sol)
```

```python
import jax
import jax.numpy as jnp
from jax import lax
from jax.experimental import pallas as pl
from jax.experimental.pallas import tpu as pltpu
from jax.sharding import PartitionSpec as P

MESH = pl.DeviceIdType.MESH
ORDER = 4
W = 48
F32 = jnp.float32
I32 = jnp.int32
ROUND_FIELDS = (7, 4) + (1,) * 9


def lane_pick(row, lo):
    return jnp.take_along_axis(jnp.broadcast_to(row, (8, 128)), lo, axis=1)


class Index:
    def __init__(self, idx):
        self.lo = idx & 127
        self.hi = idx >> 7

    def look(self, rows, base=0, start=None):
        out = jnp.zeros((8, 128), rows[0].dtype) if start is None else start
        for j, row in enumerate(rows):
            out = jnp.where(self.hi == base + j, lane_pick(row, self.lo), out)
        return out


def rows_of(tile, count=8):
    return [tile[j : j + 1, :] for j in range(count)]


def one_hot_pair(idx_rows, hi_count, values):
    low, high = [], [[] for _ in values]
    for j, row in enumerate(idx_rows):
        lo = jnp.broadcast_to(row & 127, (128, 128))
        low.append(jnp.where(lo == lax.broadcasted_iota(I32, (128, 128), 0), 1.0, 0.0).astype(jnp.bfloat16))
        hit = jnp.broadcast_to(row >> 7, (hi_count, 128)) == lax.broadcasted_iota(I32, (hi_count, 128), 0)
        for k, value in enumerate(values):
            picked = jnp.where(hit, jnp.broadcast_to(value[j], (hi_count, 128)), 0.0)
            high[k].append(picked.astype(jnp.bfloat16))
    return jnp.concatenate(low, 1), [jnp.concatenate(h, 1) for h in high]


def contract(a, b):
    return lax.dot_general(a, b, (((1,), (1,)), ((), ())), preferred_element_type=F32)


def kernel(old_ref, new_ref, mass_ref, rest_ref, pair_ref, live_ref, send_ref, disp_ref, mult_ref, tile_ref, list_ref, *bufs):
    rounds = len(ROUND_FIELDS)
    snd, rcv = bufs[:rounds], bufs[rounds : 2 * rounds]
    ssem, rsem = bufs[2 * rounds], bufs[2 * rounds + 1]
    ix, iy, iz = lax.axis_index("gx"), lax.axis_index("gy"), lax.axis_index("gz")
    nz = lax.axis_size("gz")
    up = lax.rem(iz + 1, nz)
    down = lax.rem(iz + nz - 1, nz)
    peers = [({"gx": 1 - ix}, 0, 2), ({"gy": 1 - iy}, 2, 2), ({"gz": up}, 4, 1), ({"gz": down}, 5, 1)]

    barrier = pltpu.get_barrier_semaphore()
    for device, _, _ in peers:
        pl.semaphore_signal(barrier, inc=1, device_id=device, device_id_type=MESH)

    def send(k, fields):
        for f, field in enumerate(fields):
            for i in range(6):
                snd[k][i, f : f + 1, :] = field[i : i + 1, :]
        copies = []
        for p, (device, row, count) in enumerate(peers):
            copy = pltpu.make_async_remote_copy(
                src_ref=snd[k].at[pl.ds(row, count)],
                dst_ref=rcv[k].at[pl.ds(row, count)],
                send_sem=ssem.at[k, p],
                recv_sem=rsem.at[k, p],
                device_id=device,
                device_id_type=MESH,
            )
            copy.start()
            copies.append(copy)
        return copies

    def arrive(k, copies):
        for copy in copies:
            copy.wait()
        return [[rcv[k][i, f : f + 1, :] for i in range(6)] for f in range(ROUND_FIELDS[k])]

    def tile(n, ref, row):
        for j in range(8):
            tile_ref[n, j : j + 1, :] = ref[row : row + 1, 128 * j : 128 * j + 128]
        return tile_ref[n]

    lane = lax.broadcasted_iota(I32, (8, 128), 1)
    sub = lax.broadcasted_iota(I32, (8, 128), 0)
    slot = sub * 128 + lane

    list_ref[...] = jnp.full((8, 128), -1, I32)
    list_ref[0:6, 0:W] = send_ref[...]
    listed = list_ref[...]
    at_list = Index(listed)
    own = [tile(n, old_ref, n) for n in range(3)] + [tile(3 + n, new_ref, n) for n in range(3)] + [mass_ref[...]]
    own_rows = [rows_of(field) for field in own]
    fields = [at_list.look(field) for field in own_rows]
    pl.semaphore_wait(barrier, 4)
    moving = send(0, fields)

    mass = own[6]
    rest = rest_ref[...]
    alive = live_ref[...] != 0
    pair_rows = [[pair_ref[r : r + 1, 128 * j : 128 * j + 128] for j in range(8)] for r in range(2)]
    for r in range(2):
        for j in range(8):
            list_ref[j : j + 1, :] = pair_rows[r][j]
        if r == 0:
            first = list_ref[...]
        else:
            second = list_ref[...]
    off = second - 1024
    block = jnp.zeros((8, 128), I32)
    for t in range(1, 6):
        block = block + jnp.where(off >= W * t, 1, 0)
    remote = off >= 0
    lane_in = off - W * block
    ghost = 1024 + 128 * block + lane_in
    target = jnp.where(remote, 1024 + 128 * (block ^ 1) + 64 + lane_in, second)
    joins = jnp.logical_and(alive, first != second)
    label = jnp.where(joins, slot + 1, 0)
    v_low = (label & 127).astype(F32)
    v_high = (label >> 7).astype(F32)
    v_high_first = v_high + jnp.where(joins, 32.0, 0.0)
    low_f, (hf1, hf2) = one_hot_pair(rows_of(first), 16, [rows_of(v_low), rows_of(v_high_first)])
    low_s, (hs1, hs2) = one_hot_pair(rows_of(target), 16, [rows_of(v_low), rows_of(v_high)])
    low = jnp.concatenate([low_f, low_s], 1)
    high = jnp.concatenate([jnp.concatenate([hf1, hs1], 1), jnp.concatenate([hf2, hs2], 1)], 0)
    summed = contract(high, low)
    code = (summed[0:16] + 128.0 * summed[16:32]).astype(I32)
    code_rows = rows_of(code)
    owner_ghost = 1024 + 128 * (sub ^ 1) + 64 + lane
    o_low = ((owner_ghost + 1) & 127).astype(F32)
    o_high = ((owner_ghost + 1) >> 7).astype(F32)
    low_l, (hl1, hl2) = one_hot_pair(rows_of(listed, 6), 16, [rows_of(o_low, 6), rows_of(o_high, 6)])
    linked = contract(jnp.concatenate([hl1, hl2], 0), low_l)
    link_rows = rows_of((linked[0:16] + 128.0 * linked[16:32]).astype(I32))

    at_first, at_second = Index(first), Index(second)
    own1 = jnp.where(joins, slot + 1 + 4096, 0)
    own2 = jnp.where(joins, slot + 1, 0)

    def other(at, mine):
        left = at.look(code_rows) - mine
        via_link = at.look(link_rows)
        number = jnp.where(left > 0, (left & 4095) - 1, via_link - 1)
        sign = jnp.where(left >= 4096, 1.0, -1.0)
        return left, number, sign

    left1, n1, sign1 = other(at_first, own1)
    left2, n2, sign2 = other(at_second, own2)
    n2 = jnp.where(remote, ghost, n2)
    at_n1, at_n2 = Index(n1), Index(n2)
    sign1 = jnp.where(n1 >= 1024, 1.0, sign1)
    sign2 = jnp.where(n2 >= 1024, 1.0, sign2)

    face_code = jnp.where(lane < 64, at_list.look(code_rows), code[8:16])
    face_code = jnp.where(sub < 6, face_code, 0)
    face = (face_code & 4095) - 1
    face_sign = jnp.where(face_code >= 4096, 1.0, -1.0)
    at_face = Index(face)

    def at_faces(field):
        return at_face.look(rows_of(field))

    from_first = [at_first.look(field) for field in own_rows]
    from_second = [at_second.look(field) for field in own_rows]
    head1 = jnp.logical_and(joins, jnp.logical_or(left1 <= 0, slot < n1))
    head2 = jnp.logical_and(jnp.logical_and(joins, jnp.logical_not(remote)), jnp.logical_or(left2 <= 0, slot < n2))
    head_values = []
    for head, flag in ((head1, 32.0), (head2, 0.0)):
        head_values.append((jnp.where(head, v_low, 0.0), jnp.where(head, v_high + flag, 0.0)))

    def high_of(idx_rows, value_rows):
        parts = []
        for row, value in zip(idx_rows, value_rows):
            hit = jnp.broadcast_to(row >> 7, (8, 128)) == sub
            parts.append(jnp.where(hit, jnp.broadcast_to(value, (8, 128)), 0.0).astype(jnp.bfloat16))
        return jnp.concatenate(parts, 1)

    heads = [
        jnp.concatenate([high_of(rows_of(first), rows_of(head_values[0][k])), high_of(rows_of(target), rows_of(head_values[1][k]))], 1)
        for k in range(2)
    ]
    headed = contract(jnp.concatenate(heads, 0), low)
    head_code = (headed[0:8] + 128.0 * headed[8:16]).astype(I32)

    ghosts = arrive(0, moving)
    at_ghost = Index(jnp.where(remote, ghost, -1))
    from_second = [at_ghost.look(ghosts[f], 8, from_second[f]) for f in range(7)]
    span = [from_first[f] - from_second[f] for f in range(6)]
    mass1, mass2 = from_first[6], from_second[6]
    scale = jnp.where(alive, 1.0, 0.0) / jnp.sqrt(mass1 + mass2)
    inverse = 1.0 / jnp.sqrt(span[0] * span[0] + span[1] * span[1] + span[2] * span[2] + 0.25)
    unit = [span[n] * inverse for n in range(3)]
    arm = [scale * unit[n] for n in range(3)]
    pull = span[3:6]
    x = scale * (unit[0] * pull[0] + unit[1] * pull[1] + unit[2] * pull[2] - rest)
    moving = send(1, [face_sign * at_faces(arm[n]) for n in range(3)] + [at_faces(x)])

    def dot3(a, b):
        return a[0] * b[0] + a[1] * b[1] + a[2] * b[2]

    mass12 = mass1 + mass2
    diag = 1.0 - dot3(arm, arm) * mass12
    arm_rows = [rows_of(arm[n]) for n in range(3)]
    via1 = [sign1 * at_n1.look(arm_rows[n]) for n in range(3)]
    via2 = [sign2 * at_n2.look(arm_rows[n]) for n in range(3)]

    def near(field):
        rows = rows_of(field)
        return at_n1.look(rows), at_n2.look(rows)

    x1, x2 = near(x)
    ghosts = arrive(1, moving)
    via1 = [mass1 * at_n1.look(ghosts[n], 8, via1[n]) for n in range(3)]
    via2 = [-mass2 * at_n2.look(ghosts[n], 8, via2[n]) for n in range(3)]
    e1 = -dot3(arm, via1)
    e2 = -dot3(arm, via2)
    x1 = at_n1.look(ghosts[3], 8, x1)
    x2 = at_n2.look(ghosts[3], 8, x2)

    k = 2

    def exchange(k, field):
        moving = send(k, [at_faces(field)])
        f1, f2 = near(field)
        ghosts = arrive(k, moving)
        return at_n1.look(ghosts[0], 8, f1), at_n2.look(ghosts[0], 8, f2), ghosts[0]

    def expansion(k, x, x1, x2):
        total = x
        for step in range(ORDER):
            x = diag * x + e1 * x1 + e2 * x2
            total = total + x
            if step < ORDER - 1:
                x1, x2, _ = exchange(k, x)
                k += 1
        return total, k

    y, k = expansion(k, x, x1, x2)
    y1, y2, _ = exchange(k, y)
    k += 1
    stretch = [pull[n] - (mass12 * arm[n] * y + via1[n] * y1 + via2[n] * y2) for n in range(3)]
    square = rest * rest
    goal = jnp.sqrt(jnp.maximum(2.0 * square - dot3(stretch, stretch), 0.25 * square))
    x = scale * (rest - goal)
    x1, x2, _ = exchange(k, x)
    k += 1
    y_second, k = expansion(k, x, x1, x2)
    z = y + y_second
    mult_ref[...] = z

    moving = send(k, [at_faces(z)])
    z_rows = rows_of(z)
    has_head = head_code > 0
    head_first = head_code >= 4096
    head_slot = (head_code & 4095) - 1
    link = jnp.concatenate(link_rows, 0) - 1
    at_head = Index(head_slot)
    next1 = at_head.look(rows_of(n1))
    next2 = at_head.look(rows_of(n2))
    turn = jnp.where(head_first, 1.0, -1.0)
    tail_slot = jnp.where(has_head, jnp.where(head_first, next1, next2), link)
    at_tail = Index(tail_slot)
    tail_sign = jnp.where(
        head_first, at_head.look(rows_of(sign1)), at_head.look(rows_of(sign2))
    )
    arm_head = [turn * at_head.look(arm_rows[n]) for n in range(3)]
    arm_tail = [at_tail.look(ghosts[n], 8, tail_sign * at_tail.look(arm_rows[n])) for n in range(3)]
    z_head = at_head.look(z_rows)
    z_tail = at_tail.look(z_rows)
    last = arrive(k, moving)
    z_tail = at_tail.look(last[0], 8, z_tail)
    for n in range(3):
        moved = -mass * (arm_head[n] * z_head + arm_tail[n] * z_tail)
        for j in range(8):
            disp_ref[n : n + 1, 128 * j : 128 * j + 128] = moved[j : j + 1, :]


def per_device(old_pos, new_pos, inv_mass, rest_length, bond_pairs, live, send_index):
    vmem = pl.BlockSpec(memory_space=pltpu.VMEM)
    rounds = len(ROUND_FIELDS)
    faces = [pltpu.VMEM((6, f, 128), F32) for f in ROUND_FIELDS]
    disp, mult = pl.pallas_call(
        kernel,
        out_shape=(jax.ShapeDtypeStruct((3, 1024), F32), jax.ShapeDtypeStruct((8, 128), F32)),
        in_specs=[vmem] * 7,
        out_specs=(vmem, vmem),
        scratch_shapes=[pltpu.VMEM((6, 8, 128), F32), pltpu.VMEM((8, 128), I32)]
        + faces
        + faces
        + [pltpu.SemaphoreType.DMA((rounds, 4)), pltpu.SemaphoreType.DMA((rounds, 4))],
        compiler_params=pltpu.CompilerParams(collective_id=0, has_side_effects=True),
        name="plincs",
    )(
        old_pos,
        new_pos,
        inv_mass.reshape(8, 128),
        rest_length.reshape(8, 128),
        bond_pairs,
        live.reshape(8, 128),
        send_index,
    )
    return disp, mult.reshape(1024)


def solution(mesh):
    in_specs = (
        P(None, ("gx", "gy", "gz")),
        P(None, ("gx", "gy", "gz")),
        P(("gx", "gy", "gz")),
        P(("gx", "gy", "gz")),
        P(None, ("gx", "gy", "gz")),
        P(("gx", "gy", "gz")),
        P(("gx", "gy", "gz"), None),
    )
    out_specs = (P(None, ("gx", "gy", "gz")), P(("gx", "gy", "gz")))
    return jax.shard_map(
        per_device, mesh=mesh, in_specs=in_specs, out_specs=out_specs, check_vma=False
    )
```

```python
import jax
import jax.numpy as jnp
from jax import lax
from jax.experimental import pallas as pl
from jax.experimental.pallas import tpu as pltpu
from jax.sharding import PartitionSpec as P

MESH = pl.DeviceIdType.MESH
ORDER = 4
W = 48
F32 = jnp.float32
I32 = jnp.int32
FIRST_PLAN = (3,)
SECOND_PLAN = (5,)
DEEP = max(FIRST_PLAN + SECOND_PLAN)
LIST_ROW = (0, 1, 4, 5, 2, 3)
STEPS = ((1, 0, 0), (1, 0, 0), (0, 0, -1), (0, 0, 1), (0, 1, 0), (0, 1, 0))


def moved_by(o, i, turn=1):
    s = STEPS[i]
    return ((o[0] + s[0]) % 2, (o[1] + s[1]) % 2, o[2] + turn * s[2])


def dist(o):
    return o[0] + o[1] + abs(o[2])


def offsets(depth):
    every = [(x, y, z) for x in range(2) for y in range(2) for z in range(-depth, depth + 1)]
    return [o for o in every if 0 < dist(o) <= depth]


def blocks(depth, levels=None):
    out = []
    for o in offsets(depth):
        need = [max(0, depth - dist(moved_by(o, i, -1))) for i in range(6)]
        if levels is not None:
            need = [min(n, levels) for n in need]
        i = 0
        while i < 6:
            j = i
            while j < 6 and need[j] == need[i]:
                j += 1
            if need[i]:
                out.append((o, need[i], i, j - i))
            i = j
    return out


class Plan:
    def __init__(self, depth, fields, levels=None):
        self.depth, self.fields = depth, fields
        self.levels = depth if levels is None else levels
        self.blocks = blocks(depth, levels)
        self.offsets = offsets(depth)

    def shapes(self):
        box = (self.levels, 6, self.fields, 128)
        return [
            pltpu.VMEM(box, F32),
            pltpu.VMEM((len(self.offsets),) + box, F32),
            pltpu.SemaphoreType.DMA((len(self.blocks),)),
            pltpu.SemaphoreType.DMA((len(self.blocks),)),
        ]


def plans():
    out = [Plan(1, 7), Plan(DEEP - 1, 1, 1), Plan(1, 4), Plan(max(FIRST_PLAN) - 1, 2)]
    out += [Plan(d, 1) for d in FIRST_PLAN]
    out += [Plan(max(SECOND_PLAN) - 1, 2), Plan(1, 1)]
    out += [Plan(d, 1) for d in SECOND_PLAN]
    return out


def lane_pick(row, lo):
    return jnp.take_along_axis(jnp.broadcast_to(row, (8, 128)), lo, axis=1)


class Index:
    def __init__(self, idx):
        self.lo = idx & 127
        self.hi = idx >> 7

    def look(self, rows, base=0, start=None):
        out = jnp.zeros((8, 128), rows[0].dtype) if start is None else start
        for j, row in enumerate(rows):
            out = jnp.where(self.hi == base + j, lane_pick(row, self.lo), out)
        return out


def rows_of(tile, count=8):
    return [tile[j : j + 1, :] for j in range(count)]


def one_hot_pair(idx_rows, hi_count, values):
    low, high = [], [[] for _ in values]
    for j, row in enumerate(idx_rows):
        lo = jnp.broadcast_to(row & 127, (128, 128))
        low.append(jnp.where(lo == lax.broadcasted_iota(I32, (128, 128), 0), 1.0, 0.0).astype(jnp.bfloat16))
        hit = jnp.broadcast_to(row >> 7, (hi_count, 128)) == lax.broadcasted_iota(I32, (hi_count, 128), 0)
        for k, value in enumerate(values):
            picked = jnp.where(hit, jnp.broadcast_to(value[j], (hi_count, 128)), 0.0)
            high[k].append(picked.astype(jnp.bfloat16))
    return jnp.concatenate(low, 1), [jnp.concatenate(h, 1) for h in high]


def contract(a, b):
    return lax.dot_general(a, b, (((1,), (1,)), ((), ())), preferred_element_type=F32)


def kernel(old_ref, new_ref, mass_ref, rest_ref, pair_ref, live_ref, send_ref, disp_ref, mult_ref, tile_ref, list_ref, pile_ref, *bufs):
    ix, iy, iz = lax.axis_index("gx"), lax.axis_index("gy"), lax.axis_index("gz")
    nz = lax.axis_size("gz")

    def peer(o):
        device = {}
        if o[0]:
            device["gx"] = 1 - ix
        if o[1]:
            device["gy"] = 1 - iy
        if o[2]:
            device["gz"] = lax.rem(iz + nz - o[2], nz)
        return device

    barrier = pltpu.get_barrier_semaphore()
    for o in offsets(DEEP):
        pl.semaphore_signal(barrier, inc=1, device_id=peer(o), device_id_type=MESH)

    todo = plans()

    count = {"tile": 6, "pile": 0}

    def fresh(name, ref, low=0):
        n = count[name]
        count[name] = n + 1 if n + 1 < ref.shape[0] else low
        return ref.at[n]

    class Exchange:
        def __init__(self, number, levels):
            self.plan = plan = todo[number]
            self.out, self.box, ssem, rsem = bufs[4 * number : 4 * number + 4]
            for f, field in enumerate(levels):
                for k, value in enumerate(field):
                    for i in range(6):
                        self.out[k, i, f : f + 1, :] = value[i : i + 1, :]
            self.copies = []
            for n, (o, deep, row, count) in enumerate(plan.blocks):
                copy = pltpu.make_async_remote_copy(
                    src_ref=self.out.at[pl.ds(0, deep), pl.ds(row, count)],
                    dst_ref=self.box.at[plan.offsets.index(o), pl.ds(0, deep), pl.ds(row, count)],
                    send_sem=ssem.at[n],
                    recv_sem=rsem.at[n],
                    device_id=peer(o),
                    device_id_type=MESH,
                )
                copy.start()
                self.copies.append(copy)

        def wait(self):
            for copy in self.copies:
                copy.wait()

        def row(self, o, k, i, f):
            if dist(o) == 0:
                return self.out[k - 1, i, f : f + 1, :]
            return self.box[self.plan.offsets.index(o), k - 1, i, f : f + 1, :]

        def faces(self, f):
            return [self.row(moved_by((0, 0, 0), i), 1, i, f) for i in range(6)]

        def arrived(self, v, k, f):
            slot_ref = fresh("tile", tile_ref, 6)
            for i in range(6):
                slot_ref[i : i + 1, :] = self.row(moved_by(v, i), k, i, f)
            return slot_ref[...]

        def ghosts(self, f, depth, exits):
            here = [(0, 0, 0)] + offsets(depth - 1)
            values = {v: [self.arrived(v, k, f) for k in range(1, depth - dist(v) + 1)] for v in here}
            for j in range(1, depth):
                for v in here:
                    if dist(v) > depth - j - 1:
                        continue
                    slot_ref = fresh("pile", pile_ref)
                    for i in range(6):
                        slot_ref[8 * i : 8 * i + 8, :] = values[moved_by(v, i)][j - 1]
                    at = exits[v]
                    for r in range(6):
                        picked = jnp.take_along_axis(slot_ref[pl.ds(r, 8, stride=8), :], at.lo, axis=1)
                        for k in range(j + 1, depth - dist(v) + 1):
                            values[v][k - 1] = jnp.where(at.hi == 8 * (k - j) + r, picked, values[v][k - 1])
            return values[(0, 0, 0)]

    def tile(n, ref, row):
        for j in range(8):
            tile_ref[n, j : j + 1, :] = ref[row : row + 1, 128 * j : 128 * j + 128]
        return tile_ref[n]

    lane = lax.broadcasted_iota(I32, (8, 128), 1)
    sub = lax.broadcasted_iota(I32, (8, 128), 0)
    slot = sub * 128 + lane

    list_ref[...] = jnp.full((8, 128), -1, I32)
    for b in range(6):
        list_ref[LIST_ROW[b] : LIST_ROW[b] + 1, 0:W] = send_ref[b : b + 1, :]
    listed = list_ref[...]
    at_list = Index(listed)
    own = [tile(n, old_ref, n) for n in range(3)] + [tile(3 + n, new_ref, n) for n in range(3)] + [mass_ref[...]]
    own_rows = [rows_of(field) for field in own]
    fields = [at_list.look(field) for field in own_rows]
    pl.semaphore_wait(barrier, len(offsets(DEEP)))
    positions = Exchange(0, [[field] for field in fields])

    mass = own[6]
    rest = rest_ref[...]
    alive = live_ref[...] != 0
    pair_rows = [[pair_ref[r : r + 1, 128 * j : 128 * j + 128] for j in range(8)] for r in range(2)]
    for r in range(2):
        for j in range(8):
            list_ref[j : j + 1, :] = pair_rows[r][j]
        if r == 0:
            first = list_ref[...]
        else:
            second = list_ref[...]
    off = second - 1024
    block = jnp.zeros((8, 128), I32)
    for t in range(1, 6):
        block = block + jnp.where(off >= W * t, 1, 0)
    remote = off >= 0
    lane_in = off - W * block
    block = block + jnp.where(block >= 4, -2, jnp.where(block >= 2, 2, 0))
    ghost = 1024 + 128 * block + lane_in
    target = jnp.where(remote, 1024 + 128 * (block ^ 1) + 64 + lane_in, second)
    joins = jnp.logical_and(alive, first != second)
    label = jnp.where(joins, slot + 1, 0)
    v_low = (label & 127).astype(F32)
    v_high = (label >> 7).astype(F32)
    v_high_first = v_high + jnp.where(joins, 32.0, 0.0)
    low_f, (hf1, hf2) = one_hot_pair(rows_of(first), 16, [rows_of(v_low), rows_of(v_high_first)])
    low_s, (hs1, hs2) = one_hot_pair(rows_of(target), 16, [rows_of(v_low), rows_of(v_high)])
    low = jnp.concatenate([low_f, low_s], 1)
    high = jnp.concatenate([jnp.concatenate([hf1, hs1], 1), jnp.concatenate([hf2, hs2], 1)], 0)
    summed = contract(high, low)
    code = (summed[0:16] + 128.0 * summed[16:32]).astype(I32)
    code_rows = rows_of(code)
    owner_ghost = 1024 + 128 * (sub ^ 1) + 64 + lane
    o_low = ((owner_ghost + 1) & 127).astype(F32)
    o_high = ((owner_ghost + 1) >> 7).astype(F32)
    low_l, (hl1, hl2) = one_hot_pair(rows_of(listed, 6), 16, [rows_of(o_low, 6), rows_of(o_high, 6)])
    linked = contract(jnp.concatenate([hl1, hl2], 0), low_l)
    link_rows = rows_of((linked[0:16] + 128.0 * linked[16:32]).astype(I32))

    at_first, at_second = Index(first), Index(second)
    own1 = jnp.where(joins, slot + 1 + 4096, 0)
    own2 = jnp.where(joins, slot + 1, 0)

    def other(at, mine):
        left = at.look(code_rows) - mine
        via_link = at.look(link_rows)
        number = jnp.where(left > 0, (left & 4095) - 1, via_link - 1)
        sign = jnp.where(left >= 4096, 1.0, -1.0)
        return left, number, sign

    left1, n1, sign1 = other(at_first, own1)
    left2, n2, sign2 = other(at_second, own2)
    n2 = jnp.where(remote, ghost, n2)
    at_n1, at_n2 = Index(n1), Index(n2)
    turn1 = jnp.where(jnp.logical_and(n1 < 1024, sign1 > 0), n1 + 4096, n1)
    turn2 = jnp.where(jnp.logical_and(n2 < 1024, sign2 > 0), n2 + 4096, n2)
    sign1 = jnp.where(n1 >= 1024, 1.0, sign1)
    sign2 = jnp.where(n2 >= 1024, 1.0, sign2)

    face_code = jnp.where(lane < 64, at_list.look(code_rows), code[8:16])
    face_code = jnp.where(sub < 6, face_code, 0)
    face = (face_code & 4095) - 1
    face_sign = jnp.where(face_code >= 4096, 1.0, -1.0)
    turn1_rows, turn2_rows = rows_of(turn1), rows_of(turn2)
    at_level, ends = [], []
    leaves = jnp.zeros((8, 128), I32)
    current, came_first = face, face_code >= 4096
    for k in range(1, DEEP + 1):
        at = Index(current)
        at_level.append(at)
        ends.append(came_first)
        follow = jnp.where(came_first, at.look(turn2_rows), at.look(turn1_rows))
        follow = jnp.where(current >= 0, follow, -1)
        outside = jnp.logical_and(follow >= 1024, follow < 4096)
        leaves = jnp.where(outside, 1024 * k + follow - 1024, leaves)
        current = jnp.where(jnp.logical_or(outside, follow < 0), -1, follow & 4095)
        came_first = follow >= 4096
    pointers = Exchange(1, [[leaves.astype(F32)]])

    def at_faces(field, depth=1):
        rows = rows_of(field)
        return [at.look(rows) for at in at_level[:depth]]

    def across(value):
        value = pltpu.roll(value, 64, axis=1)
        return jnp.where((sub & 1) == 0, pltpu.roll(value, 7, axis=0), pltpu.roll(value, 1, axis=0))

    from_first = [at_first.look(field) for field in own_rows]
    from_second = [at_second.look(field) for field in own_rows]
    head1 = jnp.logical_and(joins, jnp.logical_or(left1 <= 0, slot < n1))
    head2 = jnp.logical_and(jnp.logical_and(joins, jnp.logical_not(remote)), jnp.logical_or(left2 <= 0, slot < n2))
    head_values = []
    for head, flag in ((head1, 32.0), (head2, 0.0)):
        head_values.append((jnp.where(head, v_low, 0.0), jnp.where(head, v_high + flag, 0.0)))

    def high_of(idx_rows, value_rows):
        parts = []
        for row, value in zip(idx_rows, value_rows):
            hit = jnp.broadcast_to(row >> 7, (8, 128)) == sub
            parts.append(jnp.where(hit, jnp.broadcast_to(value, (8, 128)), 0.0).astype(jnp.bfloat16))
        return jnp.concatenate(parts, 1)

    heads = [
        jnp.concatenate([high_of(rows_of(first), rows_of(head_values[0][k])), high_of(rows_of(target), rows_of(head_values[1][k]))], 1)
        for k in range(2)
    ]
    headed = contract(jnp.concatenate(heads, 0), low)
    head_code = (headed[0:8] + 128.0 * headed[8:16]).astype(I32)

    positions.wait()
    at_ghost = Index(jnp.where(remote, ghost, -1))
    from_second = [at_ghost.look(positions.faces(f), 8, from_second[f]) for f in range(7)]
    span = [from_first[f] - from_second[f] for f in range(6)]
    mass1, mass2 = from_first[6], from_second[6]
    scale = jnp.where(alive, 1.0, 0.0) / jnp.sqrt(mass1 + mass2)
    inverse = 1.0 / jnp.sqrt(span[0] * span[0] + span[1] * span[1] + span[2] * span[2] + 0.25)
    unit = [span[n] * inverse for n in range(3)]
    arm = [scale * unit[n] for n in range(3)]
    pull = span[3:6]
    x = scale * (unit[0] * pull[0] + unit[1] * pull[1] + unit[2] * pull[2] - rest)
    arms = Exchange(2, [[face_sign * at_faces(arm[n])[0]] for n in range(3)] + [at_faces(x)])

    def dot3(a, b):
        return a[0] * b[0] + a[1] * b[1] + a[2] * b[2]

    mass12 = mass1 + mass2
    diag = 1.0 - dot3(arm, arm) * mass12
    arm_rows = [rows_of(arm[n]) for n in range(3)]
    via1 = [sign1 * at_n1.look(arm_rows[n]) for n in range(3)]
    via2 = [sign2 * at_n2.look(arm_rows[n]) for n in range(3)]

    def near(field):
        rows = rows_of(field)
        return at_n1.look(rows), at_n2.look(rows)

    x1, x2 = near(x)
    diag_levels = at_faces(diag, DEEP - 1)
    pointers.wait()
    exits = {v: Index(pointers.arrived(v, 1, 0).astype(I32)) for v in [(0, 0, 0)] + offsets(DEEP - 2)}

    arms.wait()
    arm_ghosts = [arms.faces(f) for f in range(4)]
    via1 = [mass1 * at_n1.look(arm_ghosts[n], 8, via1[n]) for n in range(3)]
    via2 = [-mass2 * at_n2.look(arm_ghosts[n], 8, via2[n]) for n in range(3)]
    e1 = -dot3(arm, via1)
    e2 = -dot3(arm, via2)
    x1 = at_n1.look(arm_ghosts[3], 8, x1)
    x2 = at_n2.look(arm_ghosts[3], 8, x2)
    total = x
    x = diag * x + e1 * x1 + e2 * x2
    total = total + x
    first_number = 4
    second_number = first_number + len(FIRST_PLAN)

    e1_rows, e2_rows = rows_of(e1), rows_of(e2)
    onward = [jnp.where(end, at.look(e2_rows), at.look(e1_rows)) for at, end in zip(at_level[: DEEP - 1], ends)]
    inward = across(jnp.where(ends[0], at_level[0].look(e1_rows), at_level[0].look(e2_rows)))

    def expansion(x, total, steps, depths, number, before=(), level1=None):
        ghosts = []
        diag_ghosts = link_ghosts = None
        for step in range(steps + 1):
            if not ghosts and (step < steps or level1 is not None):
                depth = depths[0]
                depths = depths[1:]
                moving = Exchange(number, [at_faces(x, depth)])
                number += 1
                x1, x2 = near(x)
                if diag_ghosts is None:
                    tables, deep = before
                    tables.wait()
                    diag_ghosts = tables.ghosts(0, deep, exits)
                    link_ghosts = [inward] + tables.ghosts(1, deep, exits)
                moving.wait()
                ghosts = moving.ghosts(0, depth, exits)
            else:
                x1, x2 = near(x)
            if level1 is not None:
                level1 = level1 + ghosts[0]
            if step == steps:
                break
            rows = rows_of(ghosts[0], 6)
            x1 = at_n1.look(rows, 8, x1)
            x2 = at_n2.look(rows, 8, x2)
            chain = [across(at_faces(x)[0]) if len(ghosts) > 1 else None] + ghosts
            ghosts = [
                diag_ghosts[k - 1] * chain[k] + link_ghosts[k - 1] * chain[k - 1] + link_ghosts[k] * chain[k + 1]
                for k in range(1, len(chain) - 1)
            ]
            x = diag * x + e1 * x1 + e2 * x2
            total = total + x
        return total, level1

    deep = max(FIRST_PLAN) - 1
    tables = Exchange(3, [diag_levels[:deep], onward[:deep]])
    y, _ = expansion(x, total, ORDER - 1, FIRST_PLAN, first_number, (tables, deep))
    moving = Exchange(second_number + 1, [at_faces(y)])
    deep = max(SECOND_PLAN) - 1
    tables = Exchange(second_number, [diag_levels[:deep], onward[:deep]])
    y1, y2 = near(y)
    moving.wait()
    y_ghost = moving.arrived((0, 0, 0), 1, 0)
    rows = rows_of(y_ghost, 6)
    y1 = at_n1.look(rows, 8, y1)
    y2 = at_n2.look(rows, 8, y2)
    stretch = [pull[n] - (mass12 * arm[n] * y + via1[n] * y1 + via2[n] * y2) for n in range(3)]
    square = rest * rest
    goal = jnp.sqrt(jnp.maximum(2.0 * square - dot3(stretch, stretch), 0.25 * square))
    x = scale * (rest - goal)
    z, z_ghost = expansion(x, y + x, ORDER, SECOND_PLAN, second_number + 2, (tables, deep), y_ghost)
    mult_ref[...] = z

    z_rows = rows_of(z)
    has_head = head_code > 0
    head_first = head_code >= 4096
    head_slot = (head_code & 4095) - 1
    link = jnp.concatenate(link_rows, 0) - 1
    at_head = Index(head_slot)
    next1 = at_head.look(rows_of(n1))
    next2 = at_head.look(rows_of(n2))
    turn = jnp.where(head_first, 1.0, -1.0)
    tail_slot = jnp.where(has_head, jnp.where(head_first, next1, next2), link)
    at_tail = Index(tail_slot)
    tail_sign = jnp.where(
        head_first, at_head.look(rows_of(sign1)), at_head.look(rows_of(sign2))
    )
    arm_head = [turn * at_head.look(arm_rows[n]) for n in range(3)]
    arm_tail = [at_tail.look(arm_ghosts[n], 8, tail_sign * at_tail.look(arm_rows[n])) for n in range(3)]
    z_head = at_head.look(z_rows)
    z_tail = at_tail.look(z_rows)
    z_tail = at_tail.look(rows_of(z_ghost, 6), 8, z_tail)
    for n in range(3):
        moved = -mass * (arm_head[n] * z_head + arm_tail[n] * z_tail)
        for j in range(8):
            disp_ref[n : n + 1, 128 * j : 128 * j + 128] = moved[j : j + 1, :]


def per_device(old_pos, new_pos, inv_mass, rest_length, bond_pairs, live, send_index):
    vmem = pl.BlockSpec(memory_space=pltpu.VMEM)
    disp, mult = pl.pallas_call(
        kernel,
        out_shape=(jax.ShapeDtypeStruct((3, 1024), F32), jax.ShapeDtypeStruct((8, 128), F32)),
        in_specs=[vmem] * 7,
        out_specs=(vmem, vmem),
        scratch_shapes=[pltpu.VMEM((512, 8, 128), F32), pltpu.VMEM((8, 128), I32), pltpu.VMEM((192, 64, 128), F32)]
        + [shape for plan in plans() for shape in plan.shapes()],
        compiler_params=pltpu.CompilerParams(collective_id=0, has_side_effects=True),
        name="plincs",
    )(
        old_pos,
        new_pos,
        inv_mass.reshape(8, 128),
        rest_length.reshape(8, 128),
        bond_pairs,
        live.reshape(8, 128),
        send_index,
    )
    return disp, mult.reshape(1024)


def solution(mesh):
    in_specs = (
        P(None, ("gx", "gy", "gz")),
        P(None, ("gx", "gy", "gz")),
        P(("gx", "gy", "gz")),
        P(("gx", "gy", "gz")),
        P(None, ("gx", "gy", "gz")),
        P(("gx", "gy", "gz")),
        P(("gx", "gy", "gz"), None),
    )
    out_specs = (P(None, ("gx", "gy", "gz")), P(("gx", "gy", "gz")))
    return jax.shard_map(
        per_device, mesh=mesh, in_specs=in_specs, out_specs=out_specs, check_vma=False
    )
```

```python
import jax
import jax.numpy as jnp
from jax import lax
from jax.experimental import pallas as pl
from jax.experimental.pallas import tpu as pltpu
from jax.sharding import PartitionSpec as P

MESH = pl.DeviceIdType.MESH
ORDER = 4
W = 48
F32 = jnp.float32
I32 = jnp.int32
GIVEN = (((3, 1024), F32), ((3, 1024), F32), ((8, 128), F32), ((8, 128), F32), ((2, 1024), I32), ((8, 128), I32), ((6, W), I32))
FIRST, SECOND = 4, 5
LIST_ROW = (0, 1, 4, 5, 2, 3)
STEPS = ((1, 0, 0), (1, 0, 0), (0, 0, -1), (0, 0, 1), (0, 1, 0), (0, 1, 0))


def moved_by(o, i, turn=1):
    s = STEPS[i]
    return ((o[0] + s[0]) % 2, (o[1] + s[1]) % 2, o[2] + turn * s[2])


def dist(o):
    return o[0] + o[1] + abs(o[2])


def offsets(depth):
    every = [(x, y, z) for x in range(2) for y in range(2) for z in range(-depth, depth + 1)]
    return [o for o in every if 0 < dist(o) <= depth]


def blocks(depth, levels=None):
    out = []
    for o in offsets(depth):
        need = [max(0, depth - dist(moved_by(o, i, -1))) for i in range(6)]
        if levels is not None:
            need = [min(n, levels) for n in need]
        i = 0
        while i < 6:
            j = i
            while j < 6 and need[j] == need[i]:
                j += 1
            if need[i]:
                out.append((o, need[i], i, j - i))
            i = j
    return out


class Plan:
    def __init__(self, depth, fields, levels=None):
        self.depth, self.fields = depth, fields
        self.levels = depth if levels is None else levels
        self.blocks = blocks(depth, levels)
        self.offsets = offsets(depth)

    def shapes(self):
        box = (self.levels, 6, self.fields, 128)
        return [
            pltpu.VMEM(box, F32),
            pltpu.VMEM((len(self.offsets),) + box, F32),
            pltpu.SemaphoreType.DMA((len(self.blocks),)),
            pltpu.SemaphoreType.DMA((len(self.blocks),)),
        ]


def plans():
    return [Plan(1, 7), Plan(SECOND - 1, 1, 1), Plan(1, 4), Plan(FIRST - 1, 2), Plan(FIRST, 1), Plan(1, 2), Plan(SECOND, 1)]


def lane_pick(row, lo):
    return jnp.take_along_axis(jnp.broadcast_to(row, (8, 128)), lo, axis=1)


class Index:
    def __init__(self, idx):
        self.lo = idx & 127
        self.hi = idx >> 7

    def look(self, rows, base=0, start=None):
        out = jnp.zeros((8, 128), rows[0].dtype) if start is None else start
        for j, row in enumerate(rows):
            out = jnp.where(self.hi == base + j, lane_pick(row, self.lo), out)
        return out


def rows_of(tile, count=8):
    return [tile[j : j + 1, :] for j in range(count)]


def one_hot_pair(idx_rows, hi_count, values):
    low, high = [], [[] for _ in values]
    for j, row in enumerate(idx_rows):
        lo = jnp.broadcast_to(row & 127, (128, 128))
        low.append(jnp.where(lo == lax.broadcasted_iota(I32, (128, 128), 0), 1.0, 0.0).astype(jnp.bfloat16))
        hit = jnp.broadcast_to(row >> 7, (hi_count, 128)) == lax.broadcasted_iota(I32, (hi_count, 128), 0)
        for k, value in enumerate(values):
            picked = jnp.where(hit, jnp.broadcast_to(value[j], (hi_count, 128)), 0.0)
            high[k].append(picked.astype(jnp.bfloat16))
    return jnp.concatenate(low, 1), [jnp.concatenate(h, 1) for h in high]


def contract(a, b):
    return lax.dot_general(a, b, (((1,), (1,)), ((), ())), preferred_element_type=F32)


def kernel(*refs):
    given, (disp_ref, mult_ref, tile_ref, list_ref, pile_ref), bufs = refs[:7], refs[7:12], refs[12:]
    taken, take_sem, bufs = bufs[:7], bufs[7], bufs[8:]
    ix, iy, iz = lax.axis_index("gx"), lax.axis_index("gy"), lax.axis_index("gz")
    nz = lax.axis_size("gz")

    def peer(o):
        device = {}
        if o[0]:
            device["gx"] = 1 - ix
        if o[1]:
            device["gy"] = 1 - iy
        if o[2]:
            device["gz"] = lax.rem(iz + nz - o[2], nz)
        return device

    barrier = pltpu.get_barrier_semaphore()
    for o in offsets(SECOND):
        pl.semaphore_signal(barrier, inc=1, device_id=peer(o), device_id_type=MESH)

    takes = [pltpu.make_async_copy(given[n], taken[n], take_sem.at[n]) for n in range(7)]
    for n in (6, 0, 1, 2, 4, 5, 3):
        takes[n].start()
    old_ref, new_ref, mass_ref, rest_ref, pair_ref, live_ref, send_ref = taken

    todo = plans()

    count = {"tile": 6, "pile": 0}

    def fresh(name, ref, low=0):
        n = count[name]
        count[name] = n + 1 if n + 1 < ref.shape[0] else low
        return ref.at[n]

    class Exchange:
        def __init__(self, number, levels):
            self.plan = plan = todo[number]
            self.out, self.box, ssem, rsem = bufs[4 * number : 4 * number + 4]
            for f, field in enumerate(levels):
                for k, value in enumerate(field):
                    for i in range(6):
                        self.out[k, i, f : f + 1, :] = value[i : i + 1, :]
            self.copies = []
            for n, (o, deep, row, count) in enumerate(plan.blocks):
                copy = pltpu.make_async_remote_copy(
                    src_ref=self.out.at[pl.ds(0, deep), pl.ds(row, count)],
                    dst_ref=self.box.at[plan.offsets.index(o), pl.ds(0, deep), pl.ds(row, count)],
                    send_sem=ssem.at[n],
                    recv_sem=rsem.at[n],
                    device_id=peer(o),
                    device_id_type=MESH,
                )
                copy.start()
                self.copies.append(copy)

        def wait(self):
            for copy in self.copies:
                copy.wait()

        def row(self, o, k, i, f):
            if dist(o) == 0:
                return self.out[k - 1, i, f : f + 1, :]
            return self.box[self.plan.offsets.index(o), k - 1, i, f : f + 1, :]

        def faces(self, f):
            return [self.row(moved_by((0, 0, 0), i), 1, i, f) for i in range(6)]

        def arrived(self, v, k, f):
            slot_ref = fresh("tile", tile_ref, 6)
            for i in range(6):
                slot_ref[i : i + 1, :] = self.row(moved_by(v, i), k, i, f)
            return slot_ref[...]

        def ghosts(self, f, depth, exits):
            here = [(0, 0, 0)] + offsets(depth - 1)
            values = {v: [self.arrived(v, k, f) for k in range(1, depth - dist(v) + 1)] for v in here}
            for j in range(1, depth):
                for v in here:
                    if dist(v) > depth - j - 1:
                        continue
                    slot_ref = fresh("pile", pile_ref)
                    for i in range(6):
                        slot_ref[8 * i : 8 * i + 8, :] = values[moved_by(v, i)][j - 1]
                    at = exits[v]
                    for r in range(6):
                        picked = jnp.take_along_axis(slot_ref[pl.ds(r, 8, stride=8), :], at.lo, axis=1)
                        for k in range(j + 1, depth - dist(v) + 1):
                            values[v][k - 1] = jnp.where(at.hi == 8 * (k - j) + r, picked, values[v][k - 1])
            return values[(0, 0, 0)]

    def tile(n, ref, row):
        for j in range(8):
            tile_ref[n, j : j + 1, :] = ref[row : row + 1, 128 * j : 128 * j + 128]
        return tile_ref[n]

    lane = lax.broadcasted_iota(I32, (8, 128), 1)
    sub = lax.broadcasted_iota(I32, (8, 128), 0)
    slot = sub * 128 + lane

    for take in takes:
        take.wait()
    list_ref[...] = jnp.full((8, 128), -1, I32)
    for b in range(6):
        list_ref[LIST_ROW[b] : LIST_ROW[b] + 1, 0:W] = send_ref[b : b + 1, :]
    listed = list_ref[...]
    at_list = Index(listed)
    own = [tile(n, old_ref, n) for n in range(3)] + [tile(3 + n, new_ref, n) for n in range(3)] + [mass_ref[...]]
    own_rows = [rows_of(field) for field in own]
    fields = [at_list.look(field) for field in own_rows]
    pl.semaphore_wait(barrier, len(offsets(SECOND)))
    positions = Exchange(0, [[field] for field in fields])

    mass = own[6]
    rest = rest_ref[...]
    alive = live_ref[...] != 0
    pair_rows = [[pair_ref[r : r + 1, 128 * j : 128 * j + 128] for j in range(8)] for r in range(2)]
    for r in range(2):
        for j in range(8):
            list_ref[j : j + 1, :] = pair_rows[r][j]
        if r == 0:
            first = list_ref[...]
        else:
            second = list_ref[...]
    off = second - 1024
    block = jnp.zeros((8, 128), I32)
    for t in range(1, 6):
        block = block + jnp.where(off >= W * t, 1, 0)
    remote = off >= 0
    lane_in = off - W * block
    block = block + jnp.where(block >= 4, -2, jnp.where(block >= 2, 2, 0))
    ghost = 1024 + 128 * block + lane_in
    target = jnp.where(remote, 1024 + 128 * (block ^ 1) + 64 + lane_in, second)
    joins = jnp.logical_and(alive, first != second)
    label = jnp.where(joins, slot + 1, 0)
    v_low = (label & 127).astype(F32)
    v_high = (label >> 7).astype(F32)
    v_high_first = v_high + jnp.where(joins, 32.0, 0.0)
    low_f, (hf1, hf2) = one_hot_pair(rows_of(first), 16, [rows_of(v_low), rows_of(v_high_first)])
    low_s, (hs1, hs2) = one_hot_pair(rows_of(target), 16, [rows_of(v_low), rows_of(v_high)])
    low = jnp.concatenate([low_f, low_s], 1)
    high = jnp.concatenate([jnp.concatenate([hf1, hs1], 1), jnp.concatenate([hf2, hs2], 1)], 0)
    summed = contract(high, low)
    code = (summed[0:16] + 128.0 * summed[16:32]).astype(I32)
    code_rows = rows_of(code)
    owner_ghost = 1024 + 128 * (sub ^ 1) + 64 + lane
    o_low = ((owner_ghost + 1) & 127).astype(F32)
    o_high = ((owner_ghost + 1) >> 7).astype(F32)
    low_l, (hl1, hl2) = one_hot_pair(rows_of(listed, 6), 16, [rows_of(o_low, 6), rows_of(o_high, 6)])
    linked = contract(jnp.concatenate([hl1, hl2], 0), low_l)
    link_rows = rows_of((linked[0:16] + 128.0 * linked[16:32]).astype(I32))

    at_first, at_second = Index(first), Index(second)
    own1 = jnp.where(joins, slot + 1 + 4096, 0)
    own2 = jnp.where(joins, slot + 1, 0)

    def other(at, mine):
        left = at.look(code_rows) - mine
        via_link = at.look(link_rows)
        number = jnp.where(left > 0, (left & 4095) - 1, via_link - 1)
        sign = jnp.where(left >= 4096, 1.0, -1.0)
        return left, number, sign

    left1, n1, sign1 = other(at_first, own1)
    left2, n2, sign2 = other(at_second, own2)
    n2 = jnp.where(remote, ghost, n2)
    at_n1, at_n2 = Index(n1), Index(n2)
    turn1 = jnp.where(jnp.logical_and(n1 < 1024, sign1 > 0), n1 + 4096, n1)
    turn2 = jnp.where(jnp.logical_and(n2 < 1024, sign2 > 0), n2 + 4096, n2)
    sign1 = jnp.where(n1 >= 1024, 1.0, sign1)
    sign2 = jnp.where(n2 >= 1024, 1.0, sign2)

    face_code = jnp.where(lane < 64, at_list.look(code_rows), code[8:16])
    face_code = jnp.where(sub < 6, face_code, 0)
    face = (face_code & 4095) - 1
    face_sign = jnp.where(face_code >= 4096, 1.0, -1.0)
    turn1_rows, turn2_rows = rows_of(turn1), rows_of(turn2)
    at_level, ends = [], []
    leaves = jnp.zeros((8, 128), I32)
    current, came_first = face, face_code >= 4096
    for k in range(1, SECOND + 1):
        at = Index(current)
        at_level.append(at)
        ends.append(came_first)
        follow = jnp.where(came_first, at.look(turn2_rows), at.look(turn1_rows))
        follow = jnp.where(current >= 0, follow, -1)
        outside = jnp.logical_and(follow >= 1024, follow < 4096)
        leaves = jnp.where(outside, 1024 * k + follow - 1024, leaves)
        current = jnp.where(jnp.logical_or(outside, follow < 0), -1, follow & 4095)
        came_first = follow >= 4096
    pointers = Exchange(1, [[leaves.astype(F32)]])

    def at_faces(field, depth=1):
        rows = rows_of(field)
        return [at.look(rows) for at in at_level[:depth]]

    def across(value):
        value = pltpu.roll(value, 64, axis=1)
        return jnp.where((sub & 1) == 0, pltpu.roll(value, 7, axis=0), pltpu.roll(value, 1, axis=0))

    from_first = [at_first.look(field) for field in own_rows]
    from_second = [at_second.look(field) for field in own_rows]
    head1 = jnp.logical_and(joins, jnp.logical_or(left1 <= 0, slot < n1))
    head2 = jnp.logical_and(jnp.logical_and(joins, jnp.logical_not(remote)), jnp.logical_or(left2 <= 0, slot < n2))
    head_values = []
    for head, flag in ((head1, 32.0), (head2, 0.0)):
        head_values.append((jnp.where(head, v_low, 0.0), jnp.where(head, v_high + flag, 0.0)))

    def high_of(idx_rows, value_rows):
        parts = []
        for row, value in zip(idx_rows, value_rows):
            hit = jnp.broadcast_to(row >> 7, (8, 128)) == sub
            parts.append(jnp.where(hit, jnp.broadcast_to(value, (8, 128)), 0.0).astype(jnp.bfloat16))
        return jnp.concatenate(parts, 1)

    heads = [
        jnp.concatenate([high_of(rows_of(first), rows_of(head_values[0][k])), high_of(rows_of(target), rows_of(head_values[1][k]))], 1)
        for k in range(2)
    ]
    headed = contract(jnp.concatenate(heads, 0), low)
    head_code = (headed[0:8] + 128.0 * headed[8:16]).astype(I32)

    positions.wait()
    at_ghost = Index(jnp.where(remote, ghost, -1))
    from_second = [at_ghost.look(positions.faces(f), 8, from_second[f]) for f in range(7)]
    span = [from_first[f] - from_second[f] for f in range(6)]
    mass1, mass2 = from_first[6], from_second[6]
    scale = jnp.where(alive, 1.0, 0.0) / jnp.sqrt(mass1 + mass2)
    inverse = 1.0 / jnp.sqrt(span[0] * span[0] + span[1] * span[1] + span[2] * span[2] + 0.25)
    unit = [span[n] * inverse for n in range(3)]
    arm = [scale * unit[n] for n in range(3)]
    pull = span[3:6]
    x = scale * (unit[0] * pull[0] + unit[1] * pull[1] + unit[2] * pull[2] - rest)
    arms = Exchange(2, [[face_sign * at_faces(arm[n])[0]] for n in range(3)] + [at_faces(x)])

    def dot3(a, b):
        return a[0] * b[0] + a[1] * b[1] + a[2] * b[2]

    mass12 = mass1 + mass2
    diag = 1.0 - dot3(arm, arm) * mass12
    arm_rows = [rows_of(arm[n]) for n in range(3)]
    via1 = [sign1 * at_n1.look(arm_rows[n]) for n in range(3)]
    via2 = [sign2 * at_n2.look(arm_rows[n]) for n in range(3)]

    def near(field):
        rows = rows_of(field)
        return at_n1.look(rows), at_n2.look(rows)

    x1, x2 = near(x)
    diag_levels = at_faces(diag, SECOND - 1)
    pointers.wait()
    exits = {v: Index(pointers.arrived(v, 1, 0).astype(I32)) for v in [(0, 0, 0)] + offsets(SECOND - 2)}

    arms.wait()
    arm_ghosts = [arms.faces(f) for f in range(4)]
    via1 = [mass1 * at_n1.look(arm_ghosts[n], 8, via1[n]) for n in range(3)]
    via2 = [-mass2 * at_n2.look(arm_ghosts[n], 8, via2[n]) for n in range(3)]
    e1 = -dot3(arm, via1)
    e2 = -dot3(arm, via2)
    x1 = at_n1.look(arm_ghosts[3], 8, x1)
    x2 = at_n2.look(arm_ghosts[3], 8, x2)
    e1_rows, e2_rows = rows_of(e1), rows_of(e2)
    onward = [jnp.where(end, at.look(e2_rows), at.look(e1_rows)) for at, end in zip(at_level[: SECOND - 1], ends)]
    inward = across(jnp.where(ends[0], at_level[0].look(e1_rows), at_level[0].look(e2_rows)))

    def step(x, x1, x2, ghosts, diag_ghosts, link_ghosts):
        rows = rows_of(ghosts[0], 6)
        x1 = at_n1.look(rows, 8, x1)
        x2 = at_n2.look(rows, 8, x2)
        chain = [across(at_faces(x)[0]) if len(ghosts) > 1 else None] + ghosts
        ghosts = [
            diag_ghosts[k - 1] * chain[k] + link_ghosts[k - 1] * chain[k - 1] + link_ghosts[k] * chain[k + 1]
            for k in range(1, len(chain) - 1)
        ]
        return diag * x + e1 * x1 + e2 * x2, ghosts

    y = x
    y_ghost = jnp.concatenate(arm_ghosts[3] + arm_ghosts[3][:2], 0)
    x, _ = step(x, x1, x2, [y_ghost], None, None)
    moving = Exchange(4, [at_faces(x, FIRST)])
    tables = Exchange(3, [diag_levels[: FIRST - 1], onward[: FIRST - 1]])
    x1, x2 = near(x)
    tables.wait()
    diag_ghosts = tables.ghosts(0, FIRST - 1, exits)
    link_ghosts = [inward] + tables.ghosts(1, FIRST - 1, exits)
    moving.wait()
    ghosts = moving.ghosts(0, FIRST, exits)
    for n in range(ORDER):
        y = y + x
        y_ghost = y_ghost + ghosts[0]
        if n == ORDER - 1:
            break
        x, ghosts = step(x, x1, x2, ghosts, diag_ghosts, link_ghosts)
        x1, x2 = near(x)

    y1, y2 = near(y)
    rows = rows_of(y_ghost, 6)
    y1 = at_n1.look(rows, 8, y1)
    y2 = at_n2.look(rows, 8, y2)
    stretch = [pull[n] - (mass12 * arm[n] * y + via1[n] * y1 + via2[n] * y2) for n in range(3)]
    square = rest * rest
    goal = jnp.sqrt(jnp.maximum(2.0 * square - dot3(stretch, stretch), 0.25 * square))
    x = scale * (rest - goal)
    moving = Exchange(6, [at_faces(x, SECOND)])

    at_exit = Index(leaves)

    def resolved(value, ghost_levels):
        for t in range(1, SECOND - 1):
            value = at_exit.look(rows_of(ghost_levels[SECOND - 2 - t], 6), 8 * t, value)
        return value

    last = Exchange(5, [[resolved(diag_levels[-1], diag_ghosts)], [resolved(onward[-1], link_ghosts[1:])]])
    x1, x2 = near(x)
    last.wait()
    diag_ghosts = diag_ghosts + [last.arrived((0, 0, 0), 1, 0)]
    link_ghosts = link_ghosts + [last.arrived((0, 0, 0), 1, 1)]
    moving.wait()
    ghosts = moving.ghosts(0, SECOND, exits)
    z, z_ghost = y, y_ghost
    for n in range(ORDER + 1):
        z = z + x
        z_ghost = z_ghost + ghosts[0]
        if n == ORDER:
            break
        x, ghosts = step(x, x1, x2, ghosts, diag_ghosts, link_ghosts)
        x1, x2 = near(x)
    mult_ref[...] = z

    z_rows = rows_of(z)
    has_head = head_code > 0
    head_first = head_code >= 4096
    head_slot = (head_code & 4095) - 1
    link = jnp.concatenate(link_rows, 0) - 1
    at_head = Index(head_slot)
    next1 = at_head.look(rows_of(n1))
    next2 = at_head.look(rows_of(n2))
    turn = jnp.where(head_first, 1.0, -1.0)
    tail_slot = jnp.where(has_head, jnp.where(head_first, next1, next2), link)
    at_tail = Index(tail_slot)
    tail_sign = jnp.where(
        head_first, at_head.look(rows_of(sign1)), at_head.look(rows_of(sign2))
    )
    arm_head = [turn * at_head.look(arm_rows[n]) for n in range(3)]
    arm_tail = [at_tail.look(arm_ghosts[n], 8, tail_sign * at_tail.look(arm_rows[n])) for n in range(3)]
    z_head = at_head.look(z_rows)
    z_tail = at_tail.look(z_rows)
    z_tail = at_tail.look(rows_of(z_ghost, 6), 8, z_tail)
    for n in range(3):
        moved = -mass * (arm_head[n] * z_head + arm_tail[n] * z_tail)
        for j in range(8):
            disp_ref[n : n + 1, 128 * j : 128 * j + 128] = moved[j : j + 1, :]


def per_device(old_pos, new_pos, inv_mass, rest_length, bond_pairs, live, send_index):
    vmem = pl.BlockSpec(memory_space=pltpu.VMEM)
    disp, mult = pl.pallas_call(
        kernel,
        out_shape=(jax.ShapeDtypeStruct((3, 1024), F32), jax.ShapeDtypeStruct((8, 128), F32)),
        in_specs=[pl.BlockSpec(memory_space=pl.ANY)] * 7,
        out_specs=(vmem, vmem),
        scratch_shapes=[pltpu.VMEM((512, 8, 128), F32), pltpu.VMEM((8, 128), I32), pltpu.VMEM((192, 64, 128), F32)]
        + [pltpu.VMEM(shape, kind) for shape, kind in GIVEN]
        + [pltpu.SemaphoreType.DMA((7,))]
        + [shape for plan in plans() for shape in plan.shapes()],
        compiler_params=pltpu.CompilerParams(collective_id=0, has_side_effects=True),
        name="plincs",
    )(
        old_pos,
        new_pos,
        inv_mass.reshape(8, 128),
        rest_length.reshape(8, 128),
        bond_pairs,
        live.reshape(8, 128),
        send_index,
    )
    return disp, mult.reshape(1024)


def solution(mesh):
    in_specs = (
        P(None, ("gx", "gy", "gz")),
        P(None, ("gx", "gy", "gz")),
        P(("gx", "gy", "gz")),
        P(("gx", "gy", "gz")),
        P(None, ("gx", "gy", "gz")),
        P(("gx", "gy", "gz")),
        P(("gx", "gy", "gz"), None),
    )
    out_specs = (P(None, ("gx", "gy", "gz")), P(("gx", "gy", "gz")))
    return jax.shard_map(
        per_device, mesh=mesh, in_specs=in_specs, out_specs=out_specs, check_vma=False
    )
```

```python
import jax
import jax.numpy as jnp
from jax import lax
from jax.experimental import pallas as pl
from jax.experimental.pallas import tpu as pltpu
from jax.sharding import PartitionSpec as P

MESH = pl.DeviceIdType.MESH
ORDER = 4
W = 48
F32 = jnp.float32
I32 = jnp.int32
GIVEN = (((3, 1024), F32), ((3, 1024), F32), ((8, 128), F32), ((8, 128), F32), ((2, 1024), I32), ((8, 128), I32), ((6, W), I32))
FIRST, SECOND = 4, 5
LIST_ROW = (0, 1, 4, 5, 2, 3)
STEPS = ((1, 0, 0), (1, 0, 0), (0, 0, -1), (0, 0, 1), (0, 1, 0), (0, 1, 0))


def moved_by(o, i, turn=1):
    s = STEPS[i]
    return ((o[0] + s[0]) % 2, (o[1] + s[1]) % 2, o[2] + turn * s[2])


def dist(o):
    return o[0] + o[1] + abs(o[2])


def offsets(depth):
    every = [(x, y, z) for x in range(2) for y in range(2) for z in range(-depth, depth + 1)]
    return [o for o in every if 0 < dist(o) <= depth]


def blocks(depth, levels=None):
    out = []
    for o in offsets(depth):
        need = [max(0, depth - dist(moved_by(o, i, -1))) for i in range(6)]
        if levels is not None:
            need = [min(n, levels) for n in need]
        hit = [i for i in range(6) if need[i]]
        if hit:
            out.append((o, max(need), hit[0], hit[-1] - hit[0] + 1))
    return out


class Plan:
    def __init__(self, depth, fields, levels=None):
        self.depth, self.fields = depth, fields
        self.levels = depth if levels is None else levels
        self.blocks = blocks(depth, levels)
        self.offsets = offsets(depth)

    def shapes(self):
        box = (self.levels, 6, self.fields, 128)
        return [
            pltpu.VMEM(box, F32),
            pltpu.VMEM((len(self.offsets),) + box, F32),
            pltpu.SemaphoreType.DMA((len(self.blocks),)),
            pltpu.SemaphoreType.DMA((len(self.blocks),)),
        ]


def plans():
    return [Plan(2, 4, 1), Plan(1, 9), Plan(SECOND - 1, 1, 1), Plan(FIRST - 1, 2), Plan(FIRST, 1), Plan(1, 2), Plan(SECOND, 1)]


def lane_pick(row, lo):
    return jnp.take_along_axis(jnp.broadcast_to(row, (8, 128)), lo, axis=1)


class Index:
    def __init__(self, idx):
        self.lo = idx & 127
        self.hi = idx >> 7

    def look(self, rows, base=0, start=None):
        out = jnp.zeros((8, 128), rows[0].dtype) if start is None else start
        for j, row in enumerate(rows):
            out = jnp.where(self.hi == base + j, lane_pick(row, self.lo), out)
        return out


def rows_of(tile, count=8):
    return [tile[j : j + 1, :] for j in range(count)]


def one_hot_pair(idx_rows, hi_count, values):
    low, high = [], [[] for _ in values]
    for j, row in enumerate(idx_rows):
        lo = jnp.broadcast_to(row & 127, (128, 128))
        low.append(jnp.where(lo == lax.broadcasted_iota(I32, (128, 128), 0), 1.0, 0.0).astype(jnp.bfloat16))
        hit = jnp.broadcast_to(row >> 7, (hi_count, 128)) == lax.broadcasted_iota(I32, (hi_count, 128), 0)
        for k, value in enumerate(values):
            picked = jnp.where(hit, jnp.broadcast_to(value[j], (hi_count, 128)), 0.0)
            high[k].append(picked.astype(jnp.bfloat16))
    return jnp.concatenate(low, 1), [jnp.concatenate(h, 1) for h in high]


def contract(a, b):
    return lax.dot_general(a, b, (((1,), (1,)), ((), ())), preferred_element_type=F32)


def kernel(*refs):
    given, (disp_ref, mult_ref, tile_ref, list_ref, pile_ref), bufs = refs[:7], refs[7:12], refs[12:]
    taken, take_sem, bufs = bufs[:7], bufs[7], bufs[8:]
    ix, iy, iz = lax.axis_index("gx"), lax.axis_index("gy"), lax.axis_index("gz")
    nz = lax.axis_size("gz")

    def peer(o):
        device = {}
        if o[0]:
            device["gx"] = 1 - ix
        if o[1]:
            device["gy"] = 1 - iy
        if o[2]:
            device["gz"] = lax.rem(iz + nz - o[2], nz)
        return device

    barrier = pltpu.get_barrier_semaphore()
    for o in offsets(SECOND):
        pl.semaphore_signal(barrier, inc=1, device_id=peer(o), device_id_type=MESH)

    takes = [pltpu.make_async_copy(given[n], taken[n], take_sem.at[n]) for n in range(7)]
    for n in (6, 0, 1, 2, 4, 5, 3):
        takes[n].start()
    old_ref, new_ref, mass_ref, rest_ref, pair_ref, live_ref, send_ref = taken

    todo = plans()

    count = {"tile": 6, "pile": 0}

    def fresh(name, ref, low=0):
        n = count[name]
        count[name] = n + 1 if n + 1 < ref.shape[0] else low
        return ref.at[n]

    class Exchange:
        def __init__(self, number, levels):
            self.plan = plan = todo[number]
            self.out, self.box, ssem, rsem = bufs[4 * number : 4 * number + 4]
            for f, field in enumerate(levels):
                for k, value in enumerate(field):
                    for i in range(6):
                        self.out[k, i, f : f + 1, :] = value[i : i + 1, :]
            self.copies = []
            for n, (o, deep, row, count) in enumerate(plan.blocks):
                copy = pltpu.make_async_remote_copy(
                    src_ref=self.out.at[pl.ds(0, deep), pl.ds(row, count)],
                    dst_ref=self.box.at[plan.offsets.index(o), pl.ds(0, deep), pl.ds(row, count)],
                    send_sem=ssem.at[n],
                    recv_sem=rsem.at[n],
                    device_id=peer(o),
                    device_id_type=MESH,
                )
                copy.start()
                self.copies.append(copy)

        def wait(self):
            for copy in self.copies:
                copy.wait()

        def row(self, o, k, i, f):
            if dist(o) == 0:
                return self.out[k - 1, i, f : f + 1, :]
            return self.box[self.plan.offsets.index(o), k - 1, i, f : f + 1, :]

        def faces(self, f):
            return [self.row(moved_by((0, 0, 0), i), 1, i, f) for i in range(6)]

        def arrived(self, v, k, f):
            slot_ref = fresh("tile", tile_ref, 6)
            for i in range(6):
                slot_ref[i : i + 1, :] = self.row(moved_by(v, i), k, i, f)
            return slot_ref[...]

        def ghosts(self, f, depth, exits):
            here = [(0, 0, 0)] + offsets(depth - 1)
            values = {v: [self.arrived(v, k, f) for k in range(1, depth - dist(v) + 1)] for v in here}
            for j in range(1, depth):
                for v in here:
                    if dist(v) > depth - j - 1:
                        continue
                    slot_ref = fresh("pile", pile_ref)
                    for i in range(6):
                        slot_ref[8 * i : 8 * i + 8, :] = values[moved_by(v, i)][j - 1]
                    at = exits[v]
                    for r in range(6):
                        picked = jnp.take_along_axis(slot_ref[pl.ds(r, 8, stride=8), :], at.lo, axis=1)
                        for k in range(j + 1, depth - dist(v) + 1):
                            values[v][k - 1] = jnp.where(at.hi == 8 * (k - j) + r, picked, values[v][k - 1])
            return values[(0, 0, 0)]

    def tile(n, ref, row):
        for j in range(8):
            tile_ref[n, j : j + 1, :] = ref[row : row + 1, 128 * j : 128 * j + 128]
        return tile_ref[n]

    lane = lax.broadcasted_iota(I32, (8, 128), 1)
    sub = lax.broadcasted_iota(I32, (8, 128), 0)
    slot = sub * 128 + lane

    for take in takes:
        take.wait()
    list_ref[...] = jnp.full((8, 128), -1, I32)
    for b in range(6):
        list_ref[LIST_ROW[b] : LIST_ROW[b] + 1, 0:W] = send_ref[b : b + 1, :]
    listed = list_ref[...]
    at_list = Index(listed)
    own = [tile(n, old_ref, n) for n in range(3)] + [tile(3 + n, new_ref, n) for n in range(3)] + [mass_ref[...]]
    own_rows = [rows_of(field) for field in own]
    fields = [at_list.look(field) for field in own_rows]

    mass = own[6]
    rest = rest_ref[...]
    alive = live_ref[...] != 0
    pair_rows = [[pair_ref[r : r + 1, 128 * j : 128 * j + 128] for j in range(8)] for r in range(2)]
    for r in range(2):
        for j in range(8):
            list_ref[j : j + 1, :] = pair_rows[r][j]
        if r == 0:
            first = list_ref[...]
        else:
            second = list_ref[...]
    off = second - 1024
    block = jnp.zeros((8, 128), I32)
    for t in range(1, 6):
        block = block + jnp.where(off >= W * t, 1, 0)
    remote = off >= 0
    lane_in = off - W * block
    block = block + jnp.where(block >= 4, -2, jnp.where(block >= 2, 2, 0))
    ghost = 1024 + 128 * block + lane_in
    target = jnp.where(remote, 1024 + 128 * (block ^ 1) + 64 + lane_in, second)
    joins = jnp.logical_and(alive, first != second)
    label = jnp.where(joins, slot + 1, 0)
    v_low = (label & 127).astype(F32)
    v_high = (label >> 7).astype(F32)
    v_high_first = v_high + jnp.where(joins, 32.0, 0.0)
    low_f, (hf1, hf2) = one_hot_pair(rows_of(first), 16, [rows_of(v_low), rows_of(v_high_first)])
    low_s, (hs1, hs2) = one_hot_pair(rows_of(target), 16, [rows_of(v_low), rows_of(v_high)])
    low = jnp.concatenate([low_f, low_s], 1)
    high = jnp.concatenate([jnp.concatenate([hf1, hs1], 1), jnp.concatenate([hf2, hs2], 1)], 0)
    summed = contract(high, low)
    code = (summed[0:16] + 128.0 * summed[16:32]).astype(I32)
    code_rows = rows_of(code)
    owner_ghost = 1024 + 128 * (sub ^ 1) + 64 + lane
    o_low = ((owner_ghost + 1) & 127).astype(F32)
    o_high = ((owner_ghost + 1) >> 7).astype(F32)
    low_l, (hl1, hl2) = one_hot_pair(rows_of(listed, 6), 16, [rows_of(o_low, 6), rows_of(o_high, 6)])
    linked = contract(jnp.concatenate([hl1, hl2], 0), low_l)
    link_rows = rows_of((linked[0:16] + 128.0 * linked[16:32]).astype(I32))

    at_first, at_second = Index(first), Index(second)
    own1 = jnp.where(joins, slot + 1 + 4096, 0)
    own2 = jnp.where(joins, slot + 1, 0)

    def other(at, mine):
        left = at.look(code_rows) - mine
        via_link = at.look(link_rows)
        number = jnp.where(left > 0, (left & 4095) - 1, via_link - 1)
        sign = jnp.where(left >= 4096, 1.0, -1.0)
        return left, number, sign

    left1, n1, sign1 = other(at_first, own1)
    left2, n2, sign2 = other(at_second, own2)
    n2 = jnp.where(remote, ghost, n2)
    at_n1, at_n2 = Index(n1), Index(n2)
    turn1 = jnp.where(jnp.logical_and(n1 < 1024, sign1 > 0), n1 + 4096, n1)
    turn2 = jnp.where(jnp.logical_and(n2 < 1024, sign2 > 0), n2 + 4096, n2)
    sign1 = jnp.where(n1 >= 1024, 1.0, sign1)
    sign2 = jnp.where(n2 >= 1024, 1.0, sign2)

    face_code = jnp.where(lane < 64, at_list.look(code_rows), code[8:16])
    face_code = jnp.where(sub < 6, face_code, 0)
    face = (face_code & 4095) - 1
    turn1_rows, turn2_rows = rows_of(turn1), rows_of(turn2)
    at_level, ends = [], []
    leaves = jnp.zeros((8, 128), I32)
    current, came_first = face, face_code >= 4096
    for k in range(1, SECOND + 1):
        at = Index(current)
        at_level.append(at)
        ends.append(came_first)
        follow = jnp.where(came_first, at.look(turn2_rows), at.look(turn1_rows))
        follow = jnp.where(current >= 0, follow, -1)
        outside = jnp.logical_and(follow >= 1024, follow < 4096)
        leaves = jnp.where(outside, 1024 * k + follow - 1024, leaves)
        current = jnp.where(jnp.logical_or(outside, follow < 0), -1, follow & 4095)
        came_first = follow >= 4096
    packed = [jnp.where(lane < 64, fields[f], pltpu.roll(fields[f + 4], 64, axis=1)) for f in range(3)] + [fields[3]]
    face_rest = at_level[0].look(rows_of(rest))
    far_atom = jnp.where(ends[0], at_level[0].look(rows_of(second)), at_level[0].look(rows_of(first)))
    at_far = Index(jnp.where(face_rest > 0, far_atom, -1))
    far_fields = [at_far.look(field) for field in own_rows] + [face_rest, leaves.astype(F32)]
    pl.semaphore_wait(barrier, len(offsets(SECOND)))
    nears = Exchange(0, [[field] for field in packed])
    fars = Exchange(1, [[field] for field in far_fields])
    pointers = Exchange(2, [[leaves.astype(F32)]])

    def at_faces(field, depth=1):
        rows = rows_of(field)
        return [at.look(rows) for at in at_level[:depth]]

    def across(value):
        value = pltpu.roll(value, 64, axis=1)
        return jnp.where((sub & 1) == 0, pltpu.roll(value, 7, axis=0), pltpu.roll(value, 1, axis=0))

    from_first = [at_first.look(field) for field in own_rows]
    from_second = [at_second.look(field) for field in own_rows]
    head1 = jnp.logical_and(joins, jnp.logical_or(left1 <= 0, slot < n1))
    head2 = jnp.logical_and(jnp.logical_and(joins, jnp.logical_not(remote)), jnp.logical_or(left2 <= 0, slot < n2))
    head_values = []
    for head, flag in ((head1, 32.0), (head2, 0.0)):
        head_values.append((jnp.where(head, v_low, 0.0), jnp.where(head, v_high + flag, 0.0)))

    def high_of(idx_rows, value_rows):
        parts = []
        for row, value in zip(idx_rows, value_rows):
            hit = jnp.broadcast_to(row >> 7, (8, 128)) == sub
            parts.append(jnp.where(hit, jnp.broadcast_to(value, (8, 128)), 0.0).astype(jnp.bfloat16))
        return jnp.concatenate(parts, 1)

    heads = [
        jnp.concatenate([high_of(rows_of(first), rows_of(head_values[0][k])), high_of(rows_of(target), rows_of(head_values[1][k]))], 1)
        for k in range(2)
    ]
    headed = contract(jnp.concatenate(heads, 0), low)
    head_code = (headed[0:8] + 128.0 * headed[8:16]).astype(I32)

    nears.wait()
    at_ghost = [Index(jnp.where(remote, ghost + half, -1)) for half in (0, 64)]
    from_second = [at_ghost[f // 4].look(nears.faces(f % 4), 8, from_second[f]) for f in range(7)]
    span = [from_first[f] - from_second[f] for f in range(6)]
    mass1, mass2 = from_first[6], from_second[6]
    scale = jnp.where(alive, 1.0, 0.0) / jnp.sqrt(mass1 + mass2)
    inverse = 1.0 / jnp.sqrt(span[0] * span[0] + span[1] * span[1] + span[2] * span[2] + 0.25)
    unit = [span[n] * inverse for n in range(3)]
    arm = [scale * unit[n] for n in range(3)]
    pull = span[3:6]
    x = scale * (unit[0] * pull[0] + unit[1] * pull[1] + unit[2] * pull[2] - rest)

    def dot3(a, b):
        return a[0] * b[0] + a[1] * b[1] + a[2] * b[2]

    mass12 = mass1 + mass2
    diag = 1.0 - dot3(arm, arm) * mass12
    arm_rows = [rows_of(arm[n]) for n in range(3)]
    via1 = [sign1 * at_n1.look(arm_rows[n]) for n in range(3)]
    via2 = [sign2 * at_n2.look(arm_rows[n]) for n in range(3)]

    def near(field):
        rows = rows_of(field)
        return at_n1.look(rows), at_n2.look(rows)

    x1, x2 = near(x)
    diag_levels = at_faces(diag, SECOND - 1)

    here = (0, 0, 0)
    arrived = [nears.arrived(here, 1, f) for f in range(4)]
    near_atom = [
        jnp.where(lane < 64, arrived[f] if f < 4 else pltpu.roll(arrived[f - 4], 64, axis=1), across(fields[f])) for f in range(7)
    ]
    fars.wait()
    far_atom = [fars.arrived(here, 1, f) for f in range(8)]
    leave = fars.arrived(here, 1, 8).astype(I32)
    leave_lane = leave & 127
    leave_row = jnp.where(leave_lane < 64, leave >> 7, -1)
    seen = {v: [nears.arrived(v, 1, f) for f in range(4)] for v in offsets(1)}
    for f in range(4):
        slot_ref = fresh("pile", pile_ref)
        for i in range(6):
            slot_ref[8 * i : 8 * i + 8, :] = seen[moved_by(here, i)][f]
        for r in range(6):
            table = slot_ref[pl.ds(r, 8, stride=8), :]
            for half in range(2):
                if f + 4 * half < 7:
                    picked = jnp.take_along_axis(table, (leave_lane + 64 * half) & 127, axis=1)
                    far_atom[f + 4 * half] = jnp.where(leave_row == 8 + r, picked, far_atom[f + 4 * half])
    ghost_rest = far_atom[7]
    there = ghost_rest > 0
    ghost_span = [near_atom[f] - far_atom[f] for f in range(6)]
    ghost_scale = jnp.where(there, 1.0, 0.0) / jnp.sqrt(jnp.where(there, near_atom[6] + far_atom[6], 1.0))
    ghost_unit = [ghost_span[n] / jnp.sqrt(dot3(ghost_span[:3], ghost_span[:3]) + 0.25) for n in range(3)]
    x_ghost = ghost_scale * (dot3(ghost_unit, ghost_span[3:]) - ghost_rest)
    arm_ghosts = [rows_of(ghost_scale * ghost_unit[n], 6) for n in range(3)] + [rows_of(x_ghost, 6)]
    via1 = [mass1 * at_n1.look(arm_ghosts[n], 8, via1[n]) for n in range(3)]
    via2 = [-mass2 * at_n2.look(arm_ghosts[n], 8, via2[n]) for n in range(3)]
    e1 = -dot3(arm, via1)
    e2 = -dot3(arm, via2)
    x1 = at_n1.look(arm_ghosts[3], 8, x1)
    x2 = at_n2.look(arm_ghosts[3], 8, x2)
    e1_rows, e2_rows = rows_of(e1), rows_of(e2)
    onward = [jnp.where(end, at.look(e2_rows), at.look(e1_rows)) for at, end in zip(at_level[: SECOND - 1], ends)]
    inward = across(jnp.where(ends[0], at_level[0].look(e1_rows), at_level[0].look(e2_rows)))

    def step(x, x1, x2, ghosts, diag_ghosts, link_ghosts):
        rows = rows_of(ghosts[0], 6)
        x1 = at_n1.look(rows, 8, x1)
        x2 = at_n2.look(rows, 8, x2)
        chain = [across(at_faces(x)[0]) if len(ghosts) > 1 else None] + ghosts
        ghosts = [
            diag_ghosts[k - 1] * chain[k] + link_ghosts[k - 1] * chain[k - 1] + link_ghosts[k] * chain[k + 1]
            for k in range(1, len(chain) - 1)
        ]
        return diag * x + e1 * x1 + e2 * x2, ghosts

    y = x
    y_ghost = x_ghost
    x, _ = step(x, x1, x2, [y_ghost], None, None)
    moving = Exchange(4, [at_faces(x, FIRST)])
    tables = Exchange(3, [diag_levels[: FIRST - 1], onward[: FIRST - 1]])
    x1, x2 = near(x)
    pointers.wait()
    exits = {v: Index(pointers.arrived(v, 1, 0).astype(I32)) for v in [(0, 0, 0)] + offsets(SECOND - 2)}
    tables.wait()
    diag_ghosts = tables.ghosts(0, FIRST - 1, exits)
    link_ghosts = [inward] + tables.ghosts(1, FIRST - 1, exits)
    moving.wait()
    ghosts = moving.ghosts(0, FIRST, exits)
    for n in range(ORDER):
        y = y + x
        y_ghost = y_ghost + ghosts[0]
        if n == ORDER - 1:
            break
        x, ghosts = step(x, x1, x2, ghosts, diag_ghosts, link_ghosts)
        x1, x2 = near(x)

    y1, y2 = near(y)
    rows = rows_of(y_ghost, 6)
    y1 = at_n1.look(rows, 8, y1)
    y2 = at_n2.look(rows, 8, y2)
    stretch = [pull[n] - (mass12 * arm[n] * y + via1[n] * y1 + via2[n] * y2) for n in range(3)]
    square = rest * rest
    goal = jnp.sqrt(jnp.maximum(2.0 * square - dot3(stretch, stretch), 0.25 * square))
    x = scale * (rest - goal)
    moving = Exchange(6, [at_faces(x, SECOND)])

    at_exit = Index(leaves)

    def resolved(value, ghost_levels):
        for t in range(1, SECOND - 1):
            value = at_exit.look(rows_of(ghost_levels[SECOND - 2 - t], 6), 8 * t, value)
        return value

    last = Exchange(5, [[resolved(diag_levels[-1], diag_ghosts)], [resolved(onward[-1], link_ghosts[1:])]])
    x1, x2 = near(x)
    last.wait()
    diag_ghosts = diag_ghosts + [last.arrived((0, 0, 0), 1, 0)]
    link_ghosts = link_ghosts + [last.arrived((0, 0, 0), 1, 1)]
    moving.wait()
    ghosts = moving.ghosts(0, SECOND, exits)
    z, z_ghost = y, y_ghost
    for n in range(ORDER + 1):
        z = z + x
        z_ghost = z_ghost + ghosts[0]
        if n == ORDER:
            break
        x, ghosts = step(x, x1, x2, ghosts, diag_ghosts, link_ghosts)
        x1, x2 = near(x)
    mult_ref[...] = z

    z_rows = rows_of(z)
    has_head = head_code > 0
    head_first = head_code >= 4096
    head_slot = (head_code & 4095) - 1
    link = jnp.concatenate(link_rows, 0) - 1
    at_head = Index(head_slot)
    next1 = at_head.look(rows_of(n1))
    next2 = at_head.look(rows_of(n2))
    turn = jnp.where(head_first, 1.0, -1.0)
    tail_slot = jnp.where(has_head, jnp.where(head_first, next1, next2), link)
    at_tail = Index(tail_slot)
    tail_sign = jnp.where(
        head_first, at_head.look(rows_of(sign1)), at_head.look(rows_of(sign2))
    )
    arm_head = [turn * at_head.look(arm_rows[n]) for n in range(3)]
    arm_tail = [at_tail.look(arm_ghosts[n], 8, tail_sign * at_tail.look(arm_rows[n])) for n in range(3)]
    z_head = at_head.look(z_rows)
    z_tail = at_tail.look(z_rows)
    z_tail = at_tail.look(rows_of(z_ghost, 6), 8, z_tail)
    for n in range(3):
        moved = -mass * (arm_head[n] * z_head + arm_tail[n] * z_tail)
        for j in range(8):
            disp_ref[n : n + 1, 128 * j : 128 * j + 128] = moved[j : j + 1, :]


def per_device(old_pos, new_pos, inv_mass, rest_length, bond_pairs, live, send_index):
    vmem = pl.BlockSpec(memory_space=pltpu.VMEM)
    disp, mult = pl.pallas_call(
        kernel,
        out_shape=(jax.ShapeDtypeStruct((3, 1024), F32), jax.ShapeDtypeStruct((8, 128), F32)),
        in_specs=[pl.BlockSpec(memory_space=pl.ANY)] * 7,
        out_specs=(vmem, vmem),
        scratch_shapes=[pltpu.VMEM((512, 8, 128), F32), pltpu.VMEM((8, 128), I32), pltpu.VMEM((192, 64, 128), F32)]
        + [pltpu.VMEM(shape, kind) for shape, kind in GIVEN]
        + [pltpu.SemaphoreType.DMA((7,))]
        + [shape for plan in plans() for shape in plan.shapes()],
        compiler_params=pltpu.CompilerParams(collective_id=0, has_side_effects=True),
        name="plincs",
    )(
        old_pos,
        new_pos,
        inv_mass.reshape(8, 128),
        rest_length.reshape(8, 128),
        bond_pairs,
        live.reshape(8, 128),
        send_index,
    )
    return disp, mult.reshape(1024)


def solution(mesh):
    in_specs = (
        P(None, ("gx", "gy", "gz")),
        P(None, ("gx", "gy", "gz")),
        P(("gx", "gy", "gz")),
        P(("gx", "gy", "gz")),
        P(None, ("gx", "gy", "gz")),
        P(("gx", "gy", "gz")),
        P(("gx", "gy", "gz"), None),
    )
    out_specs = (P(None, ("gx", "gy", "gz")), P(("gx", "gy", "gz")))
    return jax.shard_map(
        per_device, mesh=mesh, in_specs=in_specs, out_specs=out_specs, check_vma=False
    )
```

```python
import jax
import jax.numpy as jnp
from jax import lax
from jax.experimental import pallas as pl
from jax.experimental.pallas import tpu as pltpu
from jax.sharding import PartitionSpec as P

MESH = pl.DeviceIdType.MESH
ORDER = 4
W = 48
F32 = jnp.float32
I32 = jnp.int32
GIVEN = (((3, 1024), F32), ((3, 1024), F32), ((8, 128), F32), ((8, 128), F32), ((2, 1024), I32), ((8, 128), I32), ((6, W), I32))
FIRST, SECOND = 4, 5
LIST_ROW = (0, 1, 4, 5, 2, 3)
STEPS = ((1, 0, 0), (1, 0, 0), (0, 0, -1), (0, 0, 1), (0, 1, 0), (0, 1, 0))


def moved_by(o, i, turn=1):
    s = STEPS[i]
    return ((o[0] + s[0]) % 2, (o[1] + s[1]) % 2, o[2] + turn * s[2])


def dist(o):
    return o[0] + o[1] + abs(o[2])


def offsets(depth):
    every = [(x, y, z) for x in range(2) for y in range(2) for z in range(-depth, depth + 1)]
    return [o for o in every if 0 < dist(o) <= depth]


def blocks(depth, levels=None):
    out = []
    for o in offsets(depth):
        need = [max(0, depth - dist(moved_by(o, i, -1))) for i in range(6)]
        if levels is not None:
            need = [min(n, levels) for n in need]
        hit = [i for i in range(6) if need[i]]
        runs = []
        for i in hit:
            if runs and runs[-1][2] + runs[-1][3] == i and runs[-1][1] == need[i]:
                runs[-1] = (o, need[i], runs[-1][2], runs[-1][3] + 1)
            else:
                runs.append((o, need[i], i, 1))
        if hit:
            whole = (o, max(need), hit[0], hit[-1] - hit[0] + 1)
            spare = whole[1] * whole[3] - sum(need)
            out += runs if len(runs) > 1 and spare >= (4 if len(runs) == 2 else 10) else [whole]
    return out


class Plan:
    def __init__(self, depth, fields, levels=None):
        self.depth, self.fields = depth, fields
        self.levels = depth if levels is None else levels
        self.blocks = blocks(depth, levels)
        self.offsets = offsets(depth)

    def shapes(self):
        box = (self.levels, 6, self.fields, 128)
        return [
            pltpu.VMEM(box, F32),
            pltpu.VMEM((len(self.offsets),) + box, F32),
            pltpu.SemaphoreType.DMA((len(self.blocks),)),
            pltpu.SemaphoreType.DMA((len(self.blocks),)),
        ]


def plans():
    return [Plan(2, 4, 1), Plan(1, 9), Plan(SECOND - 1, 1, 1), Plan(FIRST - 1, 2), Plan(FIRST, 1), Plan(1, 2), Plan(SECOND, 1)]


def lane_pick(row, lo):
    return jnp.take_along_axis(jnp.broadcast_to(row, (8, 128)), lo, axis=1)


class Index:
    def __init__(self, idx):
        self.lo = idx & 127
        self.hi = idx >> 7

    def look(self, rows, base=0, start=None):
        out = jnp.zeros((8, 128), rows[0].dtype) if start is None else start
        for j, row in enumerate(rows):
            out = jnp.where(self.hi == base + j, lane_pick(row, self.lo), out)
        return out


def rows_of(tile, count=8):
    return [tile[j : j + 1, :] for j in range(count)]


def one_hot_pair(idx_rows, hi_count, values):
    low, high = [], [[] for _ in values]
    for j, row in enumerate(idx_rows):
        lo = jnp.broadcast_to(row & 127, (128, 128))
        low.append(jnp.where(lo == lax.broadcasted_iota(I32, (128, 128), 0), 1.0, 0.0).astype(jnp.bfloat16))
        hit = jnp.broadcast_to(row >> 7, (hi_count, 128)) == lax.broadcasted_iota(I32, (hi_count, 128), 0)
        for k, value in enumerate(values):
            picked = jnp.where(hit, jnp.broadcast_to(value[j], (hi_count, 128)), 0.0)
            high[k].append(picked.astype(jnp.bfloat16))
    return jnp.concatenate(low, 1), [jnp.concatenate(h, 1) for h in high]


def contract(a, b):
    return lax.dot_general(a, b, (((1,), (1,)), ((), ())), preferred_element_type=F32)


def kernel(*refs):
    given, (disp_ref, mult_ref, tile_ref, list_ref, pile_ref), bufs = refs[:7], refs[7:12], refs[12:]
    taken, take_sem, bufs = bufs[:7], bufs[7], bufs[8:]
    ix, iy, iz = lax.axis_index("gx"), lax.axis_index("gy"), lax.axis_index("gz")
    nz = lax.axis_size("gz")

    def peer(o):
        device = {}
        if o[0]:
            device["gx"] = 1 - ix
        if o[1]:
            device["gy"] = 1 - iy
        if o[2]:
            device["gz"] = lax.rem(iz + nz - o[2], nz)
        return device

    barrier = pltpu.get_barrier_semaphore()
    for o in offsets(SECOND):
        pl.semaphore_signal(barrier, inc=1, device_id=peer(o), device_id_type=MESH)

    takes = [pltpu.make_async_copy(given[n], taken[n], take_sem.at[n]) for n in range(7)]
    for n in (6, 0, 1, 2, 4, 5, 3):
        takes[n].start()
    old_ref, new_ref, mass_ref, rest_ref, pair_ref, live_ref, send_ref = taken

    todo = plans()

    count = {"tile": 6, "pile": 0}

    def fresh(name, ref, low=0):
        n = count[name]
        count[name] = n + 1 if n + 1 < ref.shape[0] else low
        return ref.at[n]

    class Exchange:
        def __init__(self, number, levels):
            self.plan = plan = todo[number]
            self.out, self.box, ssem, rsem = bufs[4 * number : 4 * number + 4]
            for f, field in enumerate(levels):
                for k, value in enumerate(field):
                    for i in range(6):
                        self.out[k, i, f : f + 1, :] = value[i : i + 1, :]
            self.copies = []
            for n, (o, deep, row, count) in enumerate(plan.blocks):
                copy = pltpu.make_async_remote_copy(
                    src_ref=self.out.at[pl.ds(0, deep), pl.ds(row, count)],
                    dst_ref=self.box.at[plan.offsets.index(o), pl.ds(0, deep), pl.ds(row, count)],
                    send_sem=ssem.at[n],
                    recv_sem=rsem.at[n],
                    device_id=peer(o),
                    device_id_type=MESH,
                )
                copy.start()
                self.copies.append(copy)

        def wait(self):
            for copy in self.copies:
                copy.wait()

        def row(self, o, k, i, f):
            if dist(o) == 0:
                return self.out[k - 1, i, f : f + 1, :]
            return self.box[self.plan.offsets.index(o), k - 1, i, f : f + 1, :]

        def faces(self, f):
            return [self.row(moved_by((0, 0, 0), i), 1, i, f) for i in range(6)]

        def arrived(self, v, k, f):
            slot_ref = fresh("tile", tile_ref, 6)
            for i in range(6):
                slot_ref[i : i + 1, :] = self.row(moved_by(v, i), k, i, f)
            return slot_ref[...]

        def ghosts(self, f, depth, exits):
            here = [(0, 0, 0)] + offsets(depth - 1)
            values = {v: [self.arrived(v, k, f) for k in range(1, depth - dist(v) + 1)] for v in here}
            for j in range(1, depth):
                for v in here:
                    if dist(v) > depth - j - 1:
                        continue
                    slot_ref = fresh("pile", pile_ref)
                    for i in range(6):
                        slot_ref[8 * i : 8 * i + 8, :] = values[moved_by(v, i)][j - 1]
                    at = exits[v]
                    for r in range(6):
                        picked = jnp.take_along_axis(slot_ref[pl.ds(r, 8, stride=8), :], at.lo, axis=1)
                        for k in range(j + 1, depth - dist(v) + 1):
                            values[v][k - 1] = jnp.where(at.hi == 8 * (k - j) + r, picked, values[v][k - 1])
            return values[(0, 0, 0)]

    def tile(n, ref, row):
        for j in range(8):
            tile_ref[n, j : j + 1, :] = ref[row : row + 1, 128 * j : 128 * j + 128]
        return tile_ref[n]

    lane = lax.broadcasted_iota(I32, (8, 128), 1)
    sub = lax.broadcasted_iota(I32, (8, 128), 0)
    slot = sub * 128 + lane

    for take in takes:
        take.wait()
    list_ref[...] = jnp.full((8, 128), -1, I32)
    for b in range(6):
        list_ref[LIST_ROW[b] : LIST_ROW[b] + 1, 0:W] = send_ref[b : b + 1, :]
    listed = list_ref[...]
    at_list = Index(listed)
    own = [tile(n, old_ref, n) for n in range(3)] + [tile(3 + n, new_ref, n) for n in range(3)] + [mass_ref[...]]
    own_rows = [rows_of(field) for field in own]
    fields = [at_list.look(field) for field in own_rows]

    mass = own[6]
    rest = rest_ref[...]
    alive = live_ref[...] != 0
    pair_rows = [[pair_ref[r : r + 1, 128 * j : 128 * j + 128] for j in range(8)] for r in range(2)]
    for r in range(2):
        for j in range(8):
            list_ref[j : j + 1, :] = pair_rows[r][j]
        if r == 0:
            first = list_ref[...]
        else:
            second = list_ref[...]
    off = second - 1024
    block = jnp.zeros((8, 128), I32)
    for t in range(1, 6):
        block = block + jnp.where(off >= W * t, 1, 0)
    remote = off >= 0
    lane_in = off - W * block
    block = block + jnp.where(block >= 4, -2, jnp.where(block >= 2, 2, 0))
    ghost = 1024 + 128 * block + lane_in
    target = jnp.where(remote, 1024 + 128 * (block ^ 1) + 64 + lane_in, second)
    joins = jnp.logical_and(alive, first != second)
    label = jnp.where(joins, slot + 1, 0)
    v_low = (label & 127).astype(F32)
    v_high = (label >> 7).astype(F32)
    v_high_first = v_high + jnp.where(joins, 32.0, 0.0)
    low_f, (hf1, hf2) = one_hot_pair(rows_of(first), 16, [rows_of(v_low), rows_of(v_high_first)])
    low_s, (hs1, hs2) = one_hot_pair(rows_of(target), 16, [rows_of(v_low), rows_of(v_high)])
    low = jnp.concatenate([low_f, low_s], 1)
    high = jnp.concatenate([jnp.concatenate([hf1, hs1], 1), jnp.concatenate([hf2, hs2], 1)], 0)
    summed = contract(high, low)
    code = (summed[0:16] + 128.0 * summed[16:32]).astype(I32)
    code_rows = rows_of(code)
    owner_ghost = 1024 + 128 * (sub ^ 1) + 64 + lane
    o_low = ((owner_ghost + 1) & 127).astype(F32)
    o_high = ((owner_ghost + 1) >> 7).astype(F32)
    low_l, (hl1, hl2) = one_hot_pair(rows_of(listed, 6), 16, [rows_of(o_low, 6), rows_of(o_high, 6)])
    linked = contract(jnp.concatenate([hl1, hl2], 0), low_l)
    link_rows = rows_of((linked[0:16] + 128.0 * linked[16:32]).astype(I32))

    at_first, at_second = Index(first), Index(second)
    own1 = jnp.where(joins, slot + 1 + 4096, 0)
    own2 = jnp.where(joins, slot + 1, 0)

    def other(at, mine):
        left = at.look(code_rows) - mine
        via_link = at.look(link_rows)
        number = jnp.where(left > 0, (left & 4095) - 1, via_link - 1)
        sign = jnp.where(left >= 4096, 1.0, -1.0)
        return left, number, sign

    left1, n1, sign1 = other(at_first, own1)
    left2, n2, sign2 = other(at_second, own2)
    n2 = jnp.where(remote, ghost, n2)
    at_n1, at_n2 = Index(n1), Index(n2)
    turn1 = jnp.where(jnp.logical_and(n1 < 1024, sign1 > 0), n1 + 4096, n1)
    turn2 = jnp.where(jnp.logical_and(n2 < 1024, sign2 > 0), n2 + 4096, n2)
    sign1 = jnp.where(n1 >= 1024, 1.0, sign1)
    sign2 = jnp.where(n2 >= 1024, 1.0, sign2)

    face_code = jnp.where(lane < 64, at_list.look(code_rows), code[8:16])
    face_code = jnp.where(sub < 6, face_code, 0)
    face = (face_code & 4095) - 1
    turn1_rows, turn2_rows = rows_of(turn1), rows_of(turn2)
    at_level, ends = [], []
    leaves = jnp.zeros((8, 128), I32)
    current, came_first = face, face_code >= 4096
    for k in range(1, SECOND + 1):
        at = Index(current)
        at_level.append(at)
        ends.append(came_first)
        follow = jnp.where(came_first, at.look(turn2_rows), at.look(turn1_rows))
        follow = jnp.where(current >= 0, follow, -1)
        outside = jnp.logical_and(follow >= 1024, follow < 4096)
        leaves = jnp.where(outside, 1024 * k + follow - 1024, leaves)
        current = jnp.where(jnp.logical_or(outside, follow < 0), -1, follow & 4095)
        came_first = follow >= 4096
    packed = [jnp.where(lane < 64, fields[f], pltpu.roll(fields[f + 4], 64, axis=1)) for f in range(3)] + [fields[3]]
    face_rest = at_level[0].look(rows_of(rest))
    far_atom = jnp.where(ends[0], at_level[0].look(rows_of(second)), at_level[0].look(rows_of(first)))
    at_far = Index(jnp.where(face_rest > 0, far_atom, -1))
    far_fields = [at_far.look(field) for field in own_rows] + [face_rest, leaves.astype(F32)]
    pl.semaphore_wait(barrier, len(offsets(SECOND)))
    nears = Exchange(0, [[field] for field in packed])
    fars = Exchange(1, [[field] for field in far_fields])
    pointers = Exchange(2, [[leaves.astype(F32)]])

    def at_faces(field, depth=1):
        rows = rows_of(field)
        return [at.look(rows) for at in at_level[:depth]]

    def across(value):
        value = pltpu.roll(value, 64, axis=1)
        return jnp.where((sub & 1) == 0, pltpu.roll(value, 7, axis=0), pltpu.roll(value, 1, axis=0))

    from_first = [at_first.look(field) for field in own_rows]
    from_second = [at_second.look(field) for field in own_rows]
    head1 = jnp.logical_and(joins, jnp.logical_or(left1 <= 0, slot < n1))
    head2 = jnp.logical_and(jnp.logical_and(joins, jnp.logical_not(remote)), jnp.logical_or(left2 <= 0, slot < n2))
    head_values = []
    for head, flag in ((head1, 32.0), (head2, 0.0)):
        head_values.append((jnp.where(head, v_low, 0.0), jnp.where(head, v_high + flag, 0.0)))

    def high_of(idx_rows, value_rows):
        parts = []
        for row, value in zip(idx_rows, value_rows):
            hit = jnp.broadcast_to(row >> 7, (8, 128)) == sub
            parts.append(jnp.where(hit, jnp.broadcast_to(value, (8, 128)), 0.0).astype(jnp.bfloat16))
        return jnp.concatenate(parts, 1)

    heads = [
        jnp.concatenate([high_of(rows_of(first), rows_of(head_values[0][k])), high_of(rows_of(target), rows_of(head_values[1][k]))], 1)
        for k in range(2)
    ]
    headed = contract(jnp.concatenate(heads, 0), low)
    head_code = (headed[0:8] + 128.0 * headed[8:16]).astype(I32)

    nears.wait()
    at_ghost = [Index(jnp.where(remote, ghost + half, -1)) for half in (0, 64)]
    from_second = [at_ghost[f // 4].look(nears.faces(f % 4), 8, from_second[f]) for f in range(7)]
    span = [from_first[f] - from_second[f] for f in range(6)]
    mass1, mass2 = from_first[6], from_second[6]
    scale = jnp.where(alive, 1.0, 0.0) / jnp.sqrt(mass1 + mass2)
    inverse = 1.0 / jnp.sqrt(span[0] * span[0] + span[1] * span[1] + span[2] * span[2] + 0.25)
    unit = [span[n] * inverse for n in range(3)]
    arm = [scale * unit[n] for n in range(3)]
    pull = span[3:6]
    x = scale * (unit[0] * pull[0] + unit[1] * pull[1] + unit[2] * pull[2] - rest)

    def dot3(a, b):
        return a[0] * b[0] + a[1] * b[1] + a[2] * b[2]

    mass12 = mass1 + mass2
    diag = 1.0 - dot3(arm, arm) * mass12
    arm_rows = [rows_of(arm[n]) for n in range(3)]
    via1 = [sign1 * at_n1.look(arm_rows[n]) for n in range(3)]
    via2 = [sign2 * at_n2.look(arm_rows[n]) for n in range(3)]

    def near(field):
        rows = rows_of(field)
        return at_n1.look(rows), at_n2.look(rows)

    x1, x2 = near(x)
    diag_levels = at_faces(diag, SECOND - 1)

    here = (0, 0, 0)
    arrived = [nears.arrived(here, 1, f) for f in range(4)]
    near_atom = [
        jnp.where(lane < 64, arrived[f] if f < 4 else pltpu.roll(arrived[f - 4], 64, axis=1), across(fields[f])) for f in range(7)
    ]
    fars.wait()
    far_atom = [fars.arrived(here, 1, f) for f in range(8)]
    leave = fars.arrived(here, 1, 8).astype(I32)
    leave_lane = leave & 127
    leave_row = jnp.where(leave_lane < 64, leave >> 7, -1)
    seen = {v: [nears.arrived(v, 1, f) for f in range(4)] for v in offsets(1)}
    for f in range(4):
        slot_ref = fresh("pile", pile_ref)
        for i in range(6):
            slot_ref[8 * i : 8 * i + 8, :] = seen[moved_by(here, i)][f]
        for r in range(6):
            table = slot_ref[pl.ds(r, 8, stride=8), :]
            for half in range(2):
                if f + 4 * half < 7:
                    picked = jnp.take_along_axis(table, (leave_lane + 64 * half) & 127, axis=1)
                    far_atom[f + 4 * half] = jnp.where(leave_row == 8 + r, picked, far_atom[f + 4 * half])
    ghost_rest = far_atom[7]
    there = ghost_rest > 0
    ghost_span = [near_atom[f] - far_atom[f] for f in range(6)]
    ghost_scale = jnp.where(there, 1.0, 0.0) / jnp.sqrt(jnp.where(there, near_atom[6] + far_atom[6], 1.0))
    ghost_unit = [ghost_span[n] / jnp.sqrt(dot3(ghost_span[:3], ghost_span[:3]) + 0.25) for n in range(3)]
    x_ghost = ghost_scale * (dot3(ghost_unit, ghost_span[3:]) - ghost_rest)
    arm_ghosts = [rows_of(ghost_scale * ghost_unit[n], 6) for n in range(3)] + [rows_of(x_ghost, 6)]
    via1 = [mass1 * at_n1.look(arm_ghosts[n], 8, via1[n]) for n in range(3)]
    via2 = [-mass2 * at_n2.look(arm_ghosts[n], 8, via2[n]) for n in range(3)]
    e1 = -dot3(arm, via1)
    e2 = -dot3(arm, via2)
    x1 = at_n1.look(arm_ghosts[3], 8, x1)
    x2 = at_n2.look(arm_ghosts[3], 8, x2)
    e1_rows, e2_rows = rows_of(e1), rows_of(e2)
    onward = [jnp.where(end, at.look(e2_rows), at.look(e1_rows)) for at, end in zip(at_level[: SECOND - 1], ends)]
    inward = across(jnp.where(ends[0], at_level[0].look(e1_rows), at_level[0].look(e2_rows)))

    def step(x, x1, x2, ghosts, diag_ghosts, link_ghosts):
        rows = rows_of(ghosts[0], 6)
        x1 = at_n1.look(rows, 8, x1)
        x2 = at_n2.look(rows, 8, x2)
        chain = [across(at_faces(x)[0]) if len(ghosts) > 1 else None] + ghosts
        ghosts = [
            diag_ghosts[k - 1] * chain[k] + link_ghosts[k - 1] * chain[k - 1] + link_ghosts[k] * chain[k + 1]
            for k in range(1, len(chain) - 1)
        ]
        return diag * x + e1 * x1 + e2 * x2, ghosts

    y = x
    y_ghost = x_ghost
    x, _ = step(x, x1, x2, [y_ghost], None, None)
    moving = Exchange(4, [at_faces(x, FIRST)])
    tables = Exchange(3, [diag_levels[: FIRST - 1], onward[: FIRST - 1]])
    x1, x2 = near(x)
    pointers.wait()
    exits = {v: Index(pointers.arrived(v, 1, 0).astype(I32)) for v in [(0, 0, 0)] + offsets(SECOND - 2)}
    tables.wait()
    diag_ghosts = tables.ghosts(0, FIRST - 1, exits)
    link_ghosts = [inward] + tables.ghosts(1, FIRST - 1, exits)
    moving.wait()
    ghosts = moving.ghosts(0, FIRST, exits)
    for n in range(ORDER):
        y = y + x
        y_ghost = y_ghost + ghosts[0]
        if n == ORDER - 1:
            break
        x, ghosts = step(x, x1, x2, ghosts, diag_ghosts, link_ghosts)
        x1, x2 = near(x)

    at_exit = Index(leaves)

    def resolved(value, ghost_levels):
        for t in range(1, SECOND - 1):
            value = at_exit.look(rows_of(ghost_levels[SECOND - 2 - t], 6), 8 * t, value)
        return value

    last = Exchange(5, [[resolved(diag_levels[-1], diag_ghosts)], [resolved(onward[-1], link_ghosts[1:])]])
    y1, y2 = near(y)
    rows = rows_of(y_ghost, 6)
    y1 = at_n1.look(rows, 8, y1)
    y2 = at_n2.look(rows, 8, y2)
    stretch = [pull[n] - (mass12 * arm[n] * y + via1[n] * y1 + via2[n] * y2) for n in range(3)]
    square = rest * rest
    goal = jnp.sqrt(jnp.maximum(2.0 * square - dot3(stretch, stretch), 0.25 * square))
    x = scale * (rest - goal)
    moving = Exchange(6, [at_faces(x, SECOND)])

    x1, x2 = near(x)
    last.wait()
    diag_ghosts = diag_ghosts + [last.arrived((0, 0, 0), 1, 0)]
    link_ghosts = link_ghosts + [last.arrived((0, 0, 0), 1, 1)]
    moving.wait()
    ghosts = moving.ghosts(0, SECOND, exits)
    z, z_ghost = y, y_ghost
    for n in range(ORDER + 1):
        z = z + x
        z_ghost = z_ghost + ghosts[0]
        if n == ORDER:
            break
        x, ghosts = step(x, x1, x2, ghosts, diag_ghosts, link_ghosts)
        x1, x2 = near(x)
    mult_ref[...] = z

    z_rows = rows_of(z)
    has_head = head_code > 0
    head_first = head_code >= 4096
    head_slot = (head_code & 4095) - 1
    link = jnp.concatenate(link_rows, 0) - 1
    at_head = Index(head_slot)
    next1 = at_head.look(rows_of(n1))
    next2 = at_head.look(rows_of(n2))
    turn = jnp.where(head_first, 1.0, -1.0)
    tail_slot = jnp.where(has_head, jnp.where(head_first, next1, next2), link)
    at_tail = Index(tail_slot)
    tail_sign = jnp.where(
        head_first, at_head.look(rows_of(sign1)), at_head.look(rows_of(sign2))
    )
    arm_head = [turn * at_head.look(arm_rows[n]) for n in range(3)]
    arm_tail = [at_tail.look(arm_ghosts[n], 8, tail_sign * at_tail.look(arm_rows[n])) for n in range(3)]
    z_head = at_head.look(z_rows)
    z_tail = at_tail.look(z_rows)
    z_tail = at_tail.look(rows_of(z_ghost, 6), 8, z_tail)
    for n in range(3):
        moved = -mass * (arm_head[n] * z_head + arm_tail[n] * z_tail)
        for j in range(8):
            disp_ref[n : n + 1, 128 * j : 128 * j + 128] = moved[j : j + 1, :]


def per_device(old_pos, new_pos, inv_mass, rest_length, bond_pairs, live, send_index):
    vmem = pl.BlockSpec(memory_space=pltpu.VMEM)
    disp, mult = pl.pallas_call(
        kernel,
        out_shape=(pltpu.VMEM((3, 1024), F32), pltpu.VMEM((8, 128), F32)),
        in_specs=[pl.BlockSpec(memory_space=pl.ANY)] * 7,
        out_specs=(vmem, vmem),
        scratch_shapes=[pltpu.VMEM((512, 8, 128), F32), pltpu.VMEM((8, 128), I32), pltpu.VMEM((192, 64, 128), F32)]
        + [pltpu.VMEM(shape, kind) for shape, kind in GIVEN]
        + [pltpu.SemaphoreType.DMA((7,))]
        + [shape for plan in plans() for shape in plan.shapes()],
        compiler_params=pltpu.CompilerParams(collective_id=0, has_side_effects=True),
        name="plincs",
    )(
        old_pos,
        new_pos,
        inv_mass.reshape(8, 128),
        rest_length.reshape(8, 128),
        bond_pairs,
        live.reshape(8, 128),
        send_index,
    )
    return disp, mult.reshape(1024)


def solution(mesh):
    in_specs = (
        P(None, ("gx", "gy", "gz")),
        P(None, ("gx", "gy", "gz")),
        P(("gx", "gy", "gz")),
        P(("gx", "gy", "gz")),
        P(None, ("gx", "gy", "gz")),
        P(("gx", "gy", "gz")),
        P(("gx", "gy", "gz"), None),
    )
    out_specs = (P(None, ("gx", "gy", "gz")), P(("gx", "gy", "gz")))
    return jax.shard_map(
        per_device, mesh=mesh, in_specs=in_specs, out_specs=out_specs, check_vma=False
    )
```

```python
import jax
import jax.numpy as jnp
from jax import lax
from jax.experimental import pallas as pl
from jax.experimental.pallas import tpu as pltpu
from jax.sharding import PartitionSpec as P

MESH = pl.DeviceIdType.MESH
ORDER = 4
W = 48
F32 = jnp.float32
I32 = jnp.int32
GIVEN = (((3, 1024), F32), ((3, 1024), F32), ((8, 128), F32), ((8, 128), F32), ((2, 1024), I32), ((8, 128), I32), ((6, W), I32))
FIRST, SECOND = 4, 5
LIST_ROW = (0, 1, 4, 5, 2, 3)
STEPS = ((1, 0, 0), (1, 0, 0), (0, 0, -1), (0, 0, 1), (0, 1, 0), (0, 1, 0))


def moved_by(o, i, turn=1):
    s = STEPS[i]
    return ((o[0] + s[0]) % 2, (o[1] + s[1]) % 2, o[2] + turn * s[2])


def dist(o):
    return o[0] + o[1] + abs(o[2])


def offsets(depth):
    every = [(x, y, z) for x in range(2) for y in range(2) for z in range(-depth, depth + 1)]
    return [o for o in every if 0 < dist(o) <= depth]


class Plan:
    def __init__(self, *fields):
        self.messages, self.place, self.rows = [], {}, 0
        for o in offsets(max(depth for depth, _ in fields)):
            start = self.rows
            for f, (depth, levels) in enumerate(fields):
                for i in range(6):
                    for k in range(1, min(levels, depth - dist(moved_by(o, i, -1))) + 1):
                        self.place[o, k, i, f] = self.rows
                        self.rows += 1
            self.messages.append((o, start, self.rows - start))

    def shapes(self):
        rows = pltpu.VMEM((self.rows, 1, 128), F32)
        sems = pltpu.SemaphoreType.DMA((len(self.messages),))
        return [rows, rows, sems, sems]


def plans():
    return [
        Plan(*[(2, 1)] * 4 + [(1, 1)] * 9),
        Plan((SECOND - 1, 1)),
        Plan((FIRST, FIRST), (FIRST - 1, FIRST - 1), (FIRST - 1, FIRST - 1)),
        Plan((1, 1), (1, 1)),
        Plan((SECOND, SECOND)),
    ]


def lane_pick(row, lo):
    return jnp.take_along_axis(jnp.broadcast_to(row, (8, 128)), lo, axis=1)


class Index:
    def __init__(self, idx):
        self.lo = idx & 127
        self.hi = idx >> 7

    def look(self, rows, base=0, start=None):
        out = jnp.zeros((8, 128), rows[0].dtype) if start is None else start
        for j, row in enumerate(rows):
            out = jnp.where(self.hi == base + j, lane_pick(row, self.lo), out)
        return out


def rows_of(tile, count=8):
    return [tile[j : j + 1, :] for j in range(count)]


def one_hot_pair(idx_rows, hi_count, values):
    low, high = [], [[] for _ in values]
    for j, row in enumerate(idx_rows):
        lo = jnp.broadcast_to(row & 127, (128, 128))
        low.append(jnp.where(lo == lax.broadcasted_iota(I32, (128, 128), 0), 1.0, 0.0).astype(jnp.bfloat16))
        hit = jnp.broadcast_to(row >> 7, (hi_count, 128)) == lax.broadcasted_iota(I32, (hi_count, 128), 0)
        for k, value in enumerate(values):
            picked = jnp.where(hit, jnp.broadcast_to(value[j], (hi_count, 128)), 0.0)
            high[k].append(picked.astype(jnp.bfloat16))
    return jnp.concatenate(low, 1), [jnp.concatenate(h, 1) for h in high]


def contract(a, b):
    return lax.dot_general(a, b, (((1,), (1,)), ((), ())), preferred_element_type=F32)


def kernel(*refs):
    given, (disp_ref, mult_ref, tile_ref, list_ref, pile_ref), bufs = refs[:7], refs[7:12], refs[12:]
    taken, take_sem, bufs = bufs[:7], bufs[7], bufs[8:]
    ix, iy, iz = lax.axis_index("gx"), lax.axis_index("gy"), lax.axis_index("gz")
    nz = lax.axis_size("gz")

    def peer(o):
        device = {}
        if o[0]:
            device["gx"] = 1 - ix
        if o[1]:
            device["gy"] = 1 - iy
        if o[2]:
            device["gz"] = lax.rem(iz + nz - o[2], nz)
        return device

    takes = [pltpu.make_async_copy(given[n], taken[n], take_sem.at[n]) for n in range(7)]
    for n in (6, 0, 1, 2, 4, 5, 3):
        takes[n].start()
    barrier = pltpu.get_barrier_semaphore()
    for o in offsets(SECOND):
        pl.semaphore_signal(barrier, inc=1, device_id=peer(o), device_id_type=MESH)

    old_ref, new_ref, mass_ref, rest_ref, pair_ref, live_ref, send_ref = taken

    todo = plans()

    count = {"tile": 6, "pile": 0}

    def fresh(name, ref, low=0):
        n = count[name]
        count[name] = n + 1 if n + 1 < ref.shape[0] else low
        return ref.at[n]

    class Exchange:
        def __init__(self, number, levels):
            self.plan = plan = todo[number]
            self.own = levels
            out, self.box, ssem, rsem = bufs[4 * number : 4 * number + 4]
            self.copies = []
            for n, (o, start, count) in enumerate(plan.messages):
                for (offset, k, i, f), row in plan.place.items():
                    if offset == o:
                        out[row] = levels[f][k - 1][i : i + 1, :]
            for n, (o, start, count) in enumerate(plan.messages):
                copy = pltpu.make_async_remote_copy(
                    src_ref=out.at[pl.ds(start, count)],
                    dst_ref=self.box.at[pl.ds(start, count)],
                    send_sem=ssem.at[n],
                    recv_sem=rsem.at[n],
                    device_id=peer(o),
                    device_id_type=MESH,
                )
                copy.start()
                self.copies.append(copy)

        def wait(self):
            for copy in self.copies:
                copy.wait()

        def row(self, o, k, i, f):
            if dist(o) == 0:
                return self.own[f][k - 1][i : i + 1, :]
            return self.box[self.plan.place[o, k, i, f]]

        def faces(self, f):
            return [self.row(moved_by((0, 0, 0), i), 1, i, f) for i in range(6)]

        def arrived(self, v, k, f):
            slot_ref = fresh("tile", tile_ref, 6)
            for i in range(6):
                slot_ref[i : i + 1, :] = self.row(moved_by(v, i), k, i, f)
            return slot_ref[...]

        def ghosts(self, f, depth, exits):
            here = [(0, 0, 0)] + offsets(depth - 1)
            values = {v: [self.arrived(v, k, f) for k in range(1, depth - dist(v) + 1)] for v in here}
            for j in range(1, depth):
                for v in here:
                    if dist(v) > depth - j - 1:
                        continue
                    slot_ref = fresh("pile", pile_ref)
                    for i in range(6):
                        slot_ref[8 * i : 8 * i + 8, :] = values[moved_by(v, i)][j - 1]
                    at = exits[v]
                    for r in range(6):
                        picked = jnp.take_along_axis(slot_ref[pl.ds(r, 8, stride=8), :], at.lo, axis=1)
                        for k in range(j + 1, depth - dist(v) + 1):
                            values[v][k - 1] = jnp.where(at.hi == 8 * (k - j) + r, picked, values[v][k - 1])
            return values[(0, 0, 0)]

    def tile(n, ref, row):
        for j in range(8):
            tile_ref[n, j : j + 1, :] = ref[row : row + 1, 128 * j : 128 * j + 128]
        return tile_ref[n]

    lane = lax.broadcasted_iota(I32, (8, 128), 1)
    sub = lax.broadcasted_iota(I32, (8, 128), 0)
    slot = sub * 128 + lane

    for take in takes:
        take.wait()
    list_ref[...] = jnp.full((8, 128), -1, I32)
    for b in range(6):
        list_ref[LIST_ROW[b] : LIST_ROW[b] + 1, 0:W] = send_ref[b : b + 1, :]
    listed = list_ref[...]
    at_list = Index(listed)
    own = [tile(n, old_ref, n) for n in range(3)] + [tile(3 + n, new_ref, n) for n in range(3)] + [mass_ref[...]]
    own_rows = [rows_of(field) for field in own]
    fields = [at_list.look(field) for field in own_rows]

    mass = own[6]
    rest = rest_ref[...]
    alive = live_ref[...] != 0
    pair_rows = [[pair_ref[r : r + 1, 128 * j : 128 * j + 128] for j in range(8)] for r in range(2)]
    for r in range(2):
        for j in range(8):
            list_ref[j : j + 1, :] = pair_rows[r][j]
        if r == 0:
            first = list_ref[...]
        else:
            second = list_ref[...]
    off = second - 1024
    block = jnp.zeros((8, 128), I32)
    for t in range(1, 6):
        block = block + jnp.where(off >= W * t, 1, 0)
    remote = off >= 0
    lane_in = off - W * block
    block = block + jnp.where(block >= 4, -2, jnp.where(block >= 2, 2, 0))
    ghost = 1024 + 128 * block + lane_in
    target = jnp.where(remote, 1024 + 128 * (block ^ 1) + 64 + lane_in, second)
    joins = jnp.logical_and(alive, first != second)
    label = jnp.where(joins, slot + 1, 0)
    v_low = (label & 127).astype(F32)
    v_high = (label >> 7).astype(F32)
    v_high_first = v_high + jnp.where(joins, 32.0, 0.0)
    low_f, (hf1, hf2) = one_hot_pair(rows_of(first), 16, [rows_of(v_low), rows_of(v_high_first)])
    low_s, (hs1, hs2) = one_hot_pair(rows_of(target), 16, [rows_of(v_low), rows_of(v_high)])
    low = jnp.concatenate([low_f, low_s], 1)
    high = jnp.concatenate([jnp.concatenate([hf1, hs1], 1), jnp.concatenate([hf2, hs2], 1)], 0)
    summed = contract(high, low)
    code = (summed[0:16] + 128.0 * summed[16:32]).astype(I32)
    code_rows = rows_of(code)
    owner_ghost = 1024 + 128 * (sub ^ 1) + 64 + lane
    o_low = ((owner_ghost + 1) & 127).astype(F32)
    o_high = ((owner_ghost + 1) >> 7).astype(F32)
    low_l, (hl1, hl2) = one_hot_pair(rows_of(listed, 6), 16, [rows_of(o_low, 6), rows_of(o_high, 6)])
    linked = contract(jnp.concatenate([hl1, hl2], 0), low_l)
    link_rows = rows_of((linked[0:16] + 128.0 * linked[16:32]).astype(I32))

    at_first, at_second = Index(first), Index(second)
    own1 = jnp.where(joins, slot + 1 + 4096, 0)
    own2 = jnp.where(joins, slot + 1, 0)

    def other(at, mine):
        left = at.look(code_rows) - mine
        via_link = at.look(link_rows)
        number = jnp.where(left > 0, (left & 4095) - 1, via_link - 1)
        sign = jnp.where(left >= 4096, 1.0, -1.0)
        return left, number, sign

    left1, n1, sign1 = other(at_first, own1)
    left2, n2, sign2 = other(at_second, own2)
    n2 = jnp.where(remote, ghost, n2)
    at_n1, at_n2 = Index(n1), Index(n2)
    turn1 = jnp.where(jnp.logical_and(n1 < 1024, sign1 > 0), n1 + 4096, n1)
    turn2 = jnp.where(jnp.logical_and(n2 < 1024, sign2 > 0), n2 + 4096, n2)
    sign1 = jnp.where(n1 >= 1024, 1.0, sign1)
    sign2 = jnp.where(n2 >= 1024, 1.0, sign2)

    face_code = jnp.where(lane < 64, at_list.look(code_rows), code[8:16])
    face_code = jnp.where(sub < 6, face_code, 0)
    face = (face_code & 4095) - 1
    turn1_rows, turn2_rows = rows_of(turn1), rows_of(turn2)
    at_level, ends = [], []
    leaves = jnp.zeros((8, 128), I32)
    current, came_first = face, face_code >= 4096
    for k in range(1, SECOND + 1):
        at = Index(current)
        at_level.append(at)
        ends.append(came_first)
        follow = jnp.where(came_first, at.look(turn2_rows), at.look(turn1_rows))
        follow = jnp.where(current >= 0, follow, -1)
        outside = jnp.logical_and(follow >= 1024, follow < 4096)
        leaves = jnp.where(outside, 1024 * k + follow - 1024, leaves)
        current = jnp.where(jnp.logical_or(outside, follow < 0), -1, follow & 4095)
        came_first = follow >= 4096
    packed = [jnp.where(lane < 64, fields[f], pltpu.roll(fields[f + 4], 64, axis=1)) for f in range(3)] + [fields[3]]
    face_rest = at_level[0].look(rows_of(rest))
    far_atom = jnp.where(ends[0], at_level[0].look(rows_of(second)), at_level[0].look(rows_of(first)))
    at_far = Index(jnp.where(face_rest > 0, far_atom, -1))
    far_fields = [at_far.look(field) for field in own_rows] + [face_rest, leaves.astype(F32)]
    pl.semaphore_wait(barrier, len(offsets(SECOND)))
    atoms = Exchange(0, [[field] for field in packed + far_fields])
    pointers = Exchange(1, [[leaves.astype(F32)]])

    def at_faces(field, depth=1):
        rows = rows_of(field)
        return [at.look(rows) for at in at_level[:depth]]

    def across(value):
        value = pltpu.roll(value, 64, axis=1)
        return jnp.where((sub & 1) == 0, pltpu.roll(value, 7, axis=0), pltpu.roll(value, 1, axis=0))

    from_first = [at_first.look(field) for field in own_rows]
    from_second = [at_second.look(field) for field in own_rows]
    head1 = jnp.logical_and(joins, jnp.logical_or(left1 <= 0, slot < n1))
    head2 = jnp.logical_and(jnp.logical_and(joins, jnp.logical_not(remote)), jnp.logical_or(left2 <= 0, slot < n2))
    head_values = []
    for head, flag in ((head1, 32.0), (head2, 0.0)):
        head_values.append((jnp.where(head, v_low, 0.0), jnp.where(head, v_high + flag, 0.0)))

    def high_of(idx_rows, value_rows):
        parts = []
        for row, value in zip(idx_rows, value_rows):
            hit = jnp.broadcast_to(row >> 7, (8, 128)) == sub
            parts.append(jnp.where(hit, jnp.broadcast_to(value, (8, 128)), 0.0).astype(jnp.bfloat16))
        return jnp.concatenate(parts, 1)

    heads = [
        jnp.concatenate([high_of(rows_of(first), rows_of(head_values[0][k])), high_of(rows_of(target), rows_of(head_values[1][k]))], 1)
        for k in range(2)
    ]
    headed = contract(jnp.concatenate(heads, 0), low)
    head_code = (headed[0:8] + 128.0 * headed[8:16]).astype(I32)

    atoms.wait()
    at_ghost = [Index(jnp.where(remote, ghost + half, -1)) for half in (0, 64)]
    from_second = [at_ghost[f // 4].look(atoms.faces(f % 4), 8, from_second[f]) for f in range(7)]
    span = [from_first[f] - from_second[f] for f in range(6)]
    mass1, mass2 = from_first[6], from_second[6]
    scale = jnp.where(alive, 1.0, 0.0) / jnp.sqrt(mass1 + mass2)
    inverse = 1.0 / jnp.sqrt(span[0] * span[0] + span[1] * span[1] + span[2] * span[2] + 0.25)
    unit = [span[n] * inverse for n in range(3)]
    arm = [scale * unit[n] for n in range(3)]
    pull = span[3:6]
    x = scale * (unit[0] * pull[0] + unit[1] * pull[1] + unit[2] * pull[2] - rest)

    def dot3(a, b):
        return a[0] * b[0] + a[1] * b[1] + a[2] * b[2]

    mass12 = mass1 + mass2
    diag = 1.0 - dot3(arm, arm) * mass12
    arm_rows = [rows_of(arm[n]) for n in range(3)]
    via1 = [sign1 * at_n1.look(arm_rows[n]) for n in range(3)]
    via2 = [sign2 * at_n2.look(arm_rows[n]) for n in range(3)]

    def near(field):
        rows = rows_of(field)
        return at_n1.look(rows), at_n2.look(rows)

    x1, x2 = near(x)
    diag_levels = at_faces(diag, SECOND - 1)

    here = (0, 0, 0)
    arrived = [atoms.arrived(here, 1, f) for f in range(4)]
    near_atom = [
        jnp.where(lane < 64, arrived[f] if f < 4 else pltpu.roll(arrived[f - 4], 64, axis=1), across(fields[f])) for f in range(7)
    ]
    far_atom = [atoms.arrived(here, 1, 4 + f) for f in range(8)]
    leave = atoms.arrived(here, 1, 12).astype(I32)
    leave_lane = leave & 127
    leave_row = jnp.where(leave_lane < 64, leave >> 7, -1)
    seen = {v: [atoms.arrived(v, 1, f) for f in range(4)] for v in offsets(1)}
    for f in range(4):
        slot_ref = fresh("pile", pile_ref)
        for i in range(6):
            slot_ref[8 * i : 8 * i + 8, :] = seen[moved_by(here, i)][f]
        for r in range(6):
            table = slot_ref[pl.ds(r, 8, stride=8), :]
            for half in range(2):
                if f + 4 * half < 7:
                    picked = jnp.take_along_axis(table, (leave_lane + 64 * half) & 127, axis=1)
                    far_atom[f + 4 * half] = jnp.where(leave_row == 8 + r, picked, far_atom[f + 4 * half])
    ghost_rest = far_atom[7]
    there = ghost_rest > 0
    ghost_span = [near_atom[f] - far_atom[f] for f in range(6)]
    ghost_scale = jnp.where(there, 1.0, 0.0) / jnp.sqrt(jnp.where(there, near_atom[6] + far_atom[6], 1.0))
    ghost_unit = [ghost_span[n] / jnp.sqrt(dot3(ghost_span[:3], ghost_span[:3]) + 0.25) for n in range(3)]
    x_ghost = ghost_scale * (dot3(ghost_unit, ghost_span[3:]) - ghost_rest)
    arm_ghosts = [rows_of(ghost_scale * ghost_unit[n], 6) for n in range(3)] + [rows_of(x_ghost, 6)]
    via1 = [mass1 * at_n1.look(arm_ghosts[n], 8, via1[n]) for n in range(3)]
    via2 = [-mass2 * at_n2.look(arm_ghosts[n], 8, via2[n]) for n in range(3)]
    e1 = -dot3(arm, via1)
    e2 = -dot3(arm, via2)
    x1 = at_n1.look(arm_ghosts[3], 8, x1)
    x2 = at_n2.look(arm_ghosts[3], 8, x2)
    e1_rows, e2_rows = rows_of(e1), rows_of(e2)
    onward = [jnp.where(end, at.look(e2_rows), at.look(e1_rows)) for at, end in zip(at_level[: SECOND - 1], ends)]
    inward = across(jnp.where(ends[0], at_level[0].look(e1_rows), at_level[0].look(e2_rows)))

    def step(x, x1, x2, ghosts, diag_ghosts, link_ghosts):
        rows = rows_of(ghosts[0], 6)
        x1 = at_n1.look(rows, 8, x1)
        x2 = at_n2.look(rows, 8, x2)
        chain = [across(at_faces(x)[0]) if len(ghosts) > 1 else None] + ghosts
        ghosts = [
            diag_ghosts[k - 1] * chain[k] + link_ghosts[k - 1] * chain[k - 1] + link_ghosts[k] * chain[k + 1]
            for k in range(1, len(chain) - 1)
        ]
        return diag * x + e1 * x1 + e2 * x2, ghosts

    y = x
    y_ghost = x_ghost
    x, _ = step(x, x1, x2, [y_ghost], None, None)
    moving = Exchange(2, [at_faces(x, FIRST), diag_levels[: FIRST - 1], onward[: FIRST - 1]])
    x1, x2 = near(x)
    pointers.wait()
    exits = {v: Index(pointers.arrived(v, 1, 0).astype(I32)) for v in [(0, 0, 0)] + offsets(SECOND - 2)}
    moving.wait()
    diag_ghosts = moving.ghosts(1, FIRST - 1, exits)
    link_ghosts = [inward] + moving.ghosts(2, FIRST - 1, exits)
    ghosts = moving.ghosts(0, FIRST, exits)
    for n in range(ORDER):
        y = y + x
        y_ghost = y_ghost + ghosts[0]
        if n == ORDER - 1:
            break
        x, ghosts = step(x, x1, x2, ghosts, diag_ghosts, link_ghosts)
        x1, x2 = near(x)

    at_exit = Index(leaves)

    def resolved(value, ghost_levels):
        for t in range(1, SECOND - 1):
            value = at_exit.look(rows_of(ghost_levels[SECOND - 2 - t], 6), 8 * t, value)
        return value

    last = Exchange(3, [[resolved(diag_levels[-1], diag_ghosts)], [resolved(onward[-1], link_ghosts[1:])]])
    y1, y2 = near(y)
    rows = rows_of(y_ghost, 6)
    y1 = at_n1.look(rows, 8, y1)
    y2 = at_n2.look(rows, 8, y2)
    stretch = [pull[n] - (mass12 * arm[n] * y + via1[n] * y1 + via2[n] * y2) for n in range(3)]
    square = rest * rest
    goal = jnp.sqrt(jnp.maximum(2.0 * square - dot3(stretch, stretch), 0.25 * square))
    x = scale * (rest - goal)
    moving = Exchange(4, [at_faces(x, SECOND)])

    x1, x2 = near(x)
    last.wait()
    diag_ghosts = diag_ghosts + [last.arrived((0, 0, 0), 1, 0)]
    link_ghosts = link_ghosts + [last.arrived((0, 0, 0), 1, 1)]
    moving.wait()
    ghosts = moving.ghosts(0, SECOND, exits)
    z, z_ghost = y, y_ghost
    for n in range(ORDER + 1):
        z = z + x
        z_ghost = z_ghost + ghosts[0]
        if n == ORDER:
            break
        x, ghosts = step(x, x1, x2, ghosts, diag_ghosts, link_ghosts)
        x1, x2 = near(x)
    mult_ref[...] = z

    z_rows = rows_of(z)
    has_head = head_code > 0
    head_first = head_code >= 4096
    head_slot = (head_code & 4095) - 1
    link = jnp.concatenate(link_rows, 0) - 1
    at_head = Index(head_slot)
    next1 = at_head.look(rows_of(n1))
    next2 = at_head.look(rows_of(n2))
    turn = jnp.where(head_first, 1.0, -1.0)
    tail_slot = jnp.where(has_head, jnp.where(head_first, next1, next2), link)
    at_tail = Index(tail_slot)
    tail_sign = jnp.where(
        head_first, at_head.look(rows_of(sign1)), at_head.look(rows_of(sign2))
    )
    arm_head = [turn * at_head.look(arm_rows[n]) for n in range(3)]
    arm_tail = [at_tail.look(arm_ghosts[n], 8, tail_sign * at_tail.look(arm_rows[n])) for n in range(3)]
    z_head = at_head.look(z_rows)
    z_tail = at_tail.look(z_rows)
    z_tail = at_tail.look(rows_of(z_ghost, 6), 8, z_tail)
    for n in range(3):
        moved = -mass * (arm_head[n] * z_head + arm_tail[n] * z_tail)
        for j in range(8):
            disp_ref[n : n + 1, 128 * j : 128 * j + 128] = moved[j : j + 1, :]


def per_device(old_pos, new_pos, inv_mass, rest_length, bond_pairs, live, send_index):
    vmem = pl.BlockSpec(memory_space=pltpu.VMEM)
    disp, mult = pl.pallas_call(
        kernel,
        out_shape=(pltpu.VMEM((3, 1024), F32), pltpu.VMEM((8, 128), F32)),
        in_specs=[pl.BlockSpec(memory_space=pl.ANY)] * 7,
        out_specs=(vmem, vmem),
        scratch_shapes=[pltpu.VMEM((512, 8, 128), F32), pltpu.VMEM((8, 128), I32), pltpu.VMEM((192, 64, 128), F32)]
        + [pltpu.VMEM(shape, kind) for shape, kind in GIVEN]
        + [pltpu.SemaphoreType.DMA((7,))]
        + [shape for plan in plans() for shape in plan.shapes()],
        compiler_params=pltpu.CompilerParams(collective_id=0, has_side_effects=True),
        name="plincs",
    )(
        old_pos,
        new_pos,
        inv_mass.reshape(8, 128),
        rest_length.reshape(8, 128),
        bond_pairs,
        live.reshape(8, 128),
        send_index,
    )
    return disp, mult.reshape(1024)


def solution(mesh):
    in_specs = (
        P(None, ("gx", "gy", "gz")),
        P(None, ("gx", "gy", "gz")),
        P(("gx", "gy", "gz")),
        P(("gx", "gy", "gz")),
        P(None, ("gx", "gy", "gz")),
        P(("gx", "gy", "gz")),
        P(("gx", "gy", "gz"), None),
    )
    out_specs = (P(None, ("gx", "gy", "gz")), P(("gx", "gy", "gz")))
    return jax.shard_map(
        per_device, mesh=mesh, in_specs=in_specs, out_specs=out_specs, check_vma=False
    )
```

```python
import jax
import jax.numpy as jnp
from jax import lax
from jax.experimental import pallas as pl
from jax.experimental.pallas import tpu as pltpu
from jax.sharding import PartitionSpec as P

MESH = pl.DeviceIdType.MESH
ORDER = 4
W = 48
F32 = jnp.float32
I32 = jnp.int32
GIVEN = (((3, 1024), F32), ((3, 1024), F32), ((8, 128), F32), ((8, 128), F32), ((2, 1024), I32), ((8, 128), I32), ((6, W), I32))
FIRST, SECOND = 4, 5
LIST_ROW = (0, 1, 4, 5, 2, 3)
STEPS = ((1, 0, 0), (1, 0, 0), (0, 0, -1), (0, 0, 1), (0, 1, 0), (0, 1, 0))


def moved_by(o, i, turn=1):
    s = STEPS[i]
    return ((o[0] + s[0]) % 2, (o[1] + s[1]) % 2, o[2] + turn * s[2])


def dist(o):
    return o[0] + o[1] + abs(o[2])


def offsets(depth):
    every = [(x, y, z) for x in range(2) for y in range(2) for z in range(-depth, depth + 1)]
    return [o for o in every if 0 < dist(o) <= depth]


class Plan:
    def __init__(self, *fields):
        self.messages, self.place, self.rows = [], {}, 0
        for o in sorted(offsets(max(depth for depth, _ in fields)), key=lambda o: -dist(o)):
            start = self.rows
            for f, (depth, levels) in enumerate(fields):
                for i in range(6):
                    for k in range(1, min(levels, depth - dist(moved_by(o, i, -1))) + 1):
                        self.place[o, k, i, f] = self.rows
                        self.rows += 1
            self.messages.append((o, start, self.rows - start))

    def shapes(self):
        rows = pltpu.VMEM((self.rows, 1, 128), F32)
        sems = pltpu.SemaphoreType.DMA((len(self.messages),))
        return [rows, rows, sems, sems]


def plans():
    return [
        Plan(*[(2, 1)] * 4 + [(1, 1)] * 9),
        Plan((SECOND - 1, 1)),
        Plan((FIRST, FIRST), (FIRST - 1, FIRST - 1), (FIRST - 1, FIRST - 1)),
        Plan((SECOND, SECOND), (1, 1), (1, 1)),
    ]


def lane_pick(row, lo):
    return jnp.take_along_axis(jnp.broadcast_to(row, (8, 128)), lo, axis=1)


class Index:
    def __init__(self, idx):
        self.lo = idx & 127
        self.hi = idx >> 7

    def look(self, rows, base=0, start=None):
        out = jnp.zeros((8, 128), rows[0].dtype) if start is None else start
        for j, row in enumerate(rows):
            out = jnp.where(self.hi == base + j, lane_pick(row, self.lo), out)
        return out


def rows_of(tile, count=8):
    return [tile[j : j + 1, :] for j in range(count)]


def one_hot_pair(idx_rows, hi_count, values):
    low, high = [], [[] for _ in values]
    for j, row in enumerate(idx_rows):
        lo = jnp.broadcast_to(row & 127, (128, 128))
        low.append(jnp.where(lo == lax.broadcasted_iota(I32, (128, 128), 0), 1.0, 0.0).astype(jnp.bfloat16))
        hit = jnp.broadcast_to(row >> 7, (hi_count, 128)) == lax.broadcasted_iota(I32, (hi_count, 128), 0)
        for k, value in enumerate(values):
            picked = jnp.where(hit, jnp.broadcast_to(value[j], (hi_count, 128)), 0.0)
            high[k].append(picked.astype(jnp.bfloat16))
    return jnp.concatenate(low, 1), [jnp.concatenate(h, 1) for h in high]


def contract(a, b):
    return lax.dot_general(a, b, (((1,), (1,)), ((), ())), preferred_element_type=F32)


def kernel(*refs):
    given, (disp_ref, mult_ref, tile_ref, list_ref, pile_ref), bufs = refs[:7], refs[7:12], refs[12:]
    taken, take_sem, bufs = bufs[:7], bufs[7], bufs[8:]
    ix, iy, iz = lax.axis_index("gx"), lax.axis_index("gy"), lax.axis_index("gz")
    nz = lax.axis_size("gz")

    def peer(o):
        device = {}
        if o[0]:
            device["gx"] = 1 - ix
        if o[1]:
            device["gy"] = 1 - iy
        if o[2]:
            device["gz"] = lax.rem(iz + nz - o[2], nz)
        return device

    takes = [pltpu.make_async_copy(given[n], taken[n], take_sem.at[n]) for n in range(7)]
    for n in (6, 0, 1, 2, 4, 5, 3):
        takes[n].start()
    barrier = pltpu.get_barrier_semaphore()
    for o in offsets(SECOND):
        pl.semaphore_signal(barrier, inc=1, device_id=peer(o), device_id_type=MESH)

    old_ref, new_ref, mass_ref, rest_ref, pair_ref, live_ref, send_ref = taken

    todo = plans()

    count = {"tile": 6, "pile": 0}

    def fresh(name, ref, low=0):
        n = count[name]
        count[name] = n + 1 if n + 1 < ref.shape[0] else low
        return ref.at[n]

    class Exchange:
        def __init__(self, number, levels):
            self.plan = plan = todo[number]
            self.own = levels
            out, self.box, ssem, rsem = bufs[4 * number : 4 * number + 4]
            self.copies = []
            for n, (o, start, count) in enumerate(plan.messages):
                for (offset, k, i, f), row in plan.place.items():
                    if offset == o:
                        out[row] = levels[f][k - 1][i : i + 1, :]
            for n, (o, start, count) in enumerate(plan.messages):
                copy = pltpu.make_async_remote_copy(
                    src_ref=out.at[pl.ds(start, count)],
                    dst_ref=self.box.at[pl.ds(start, count)],
                    send_sem=ssem.at[n],
                    recv_sem=rsem.at[n],
                    device_id=peer(o),
                    device_id_type=MESH,
                )
                copy.start()
                self.copies.append(copy)

        def wait(self):
            for copy in self.copies:
                copy.wait()

        def row(self, o, k, i, f):
            if dist(o) == 0:
                return self.own[f][k - 1][i : i + 1, :]
            return self.box[self.plan.place[o, k, i, f]]

        def faces(self, f):
            return [self.row(moved_by((0, 0, 0), i), 1, i, f) for i in range(6)]

        def arrived(self, v, k, f):
            out = jnp.broadcast_to(self.row(moved_by(v, 0), k, 0, f), (8, 128))
            for i in range(1, 6):
                out = jnp.where(sub == i, self.row(moved_by(v, i), k, i, f), out)
            return out

        def ghosts(self, f, depth, exits):
            here = [(0, 0, 0)] + offsets(depth - 1)
            values = {v: [self.arrived(v, k, f) for k in range(1, depth - dist(v) + 1)] for v in here}
            for j in range(1, depth):
                for v in here:
                    if dist(v) > depth - j - 1:
                        continue
                    slot_ref = fresh("pile", pile_ref)
                    for i in range(6):
                        slot_ref[8 * i : 8 * i + 8, :] = values[moved_by(v, i)][j - 1]
                    at = exits[v]
                    for r in range(6):
                        picked = jnp.take_along_axis(slot_ref[pl.ds(r, 8, stride=8), :], at.lo, axis=1)
                        for k in range(j + 1, depth - dist(v) + 1):
                            values[v][k - 1] = jnp.where(at.hi == 8 * (k - j) + r, picked, values[v][k - 1])
            return values[(0, 0, 0)]

    def tile(n, ref, row):
        for j in range(8):
            tile_ref[n, j : j + 1, :] = ref[row : row + 1, 128 * j : 128 * j + 128]
        return tile_ref[n]

    lane = lax.broadcasted_iota(I32, (8, 128), 1)
    sub = lax.broadcasted_iota(I32, (8, 128), 0)
    slot = sub * 128 + lane

    for take in takes:
        take.wait()
    list_ref[...] = jnp.full((8, 128), -1, I32)
    for b in range(6):
        list_ref[LIST_ROW[b] : LIST_ROW[b] + 1, 0:W] = send_ref[b : b + 1, :]
    listed = list_ref[...]
    at_list = Index(listed)
    own = [tile(n, old_ref, n) for n in range(3)] + [tile(3 + n, new_ref, n) for n in range(3)] + [mass_ref[...]]
    own_rows = [rows_of(field) for field in own]
    fields = [at_list.look(field) for field in own_rows]

    mass = own[6]
    rest = rest_ref[...]
    alive = live_ref[...] != 0
    pair_rows = [[pair_ref[r : r + 1, 128 * j : 128 * j + 128] for j in range(8)] for r in range(2)]
    for r in range(2):
        for j in range(8):
            list_ref[j : j + 1, :] = pair_rows[r][j]
        if r == 0:
            first = list_ref[...]
        else:
            second = list_ref[...]
    off = second - 1024
    block = jnp.zeros((8, 128), I32)
    for t in range(1, 6):
        block = block + jnp.where(off >= W * t, 1, 0)
    remote = off >= 0
    lane_in = off - W * block
    block = block + jnp.where(block >= 4, -2, jnp.where(block >= 2, 2, 0))
    ghost = 1024 + 128 * block + lane_in
    target = jnp.where(remote, 1024 + 128 * (block ^ 1) + 64 + lane_in, second)
    joins = jnp.logical_and(alive, first != second)
    label = jnp.where(joins, slot + 1, 0)
    v_low = (label & 127).astype(F32)
    v_high = (label >> 7).astype(F32)
    v_high_first = v_high + jnp.where(joins, 32.0, 0.0)
    low_f, (hf1, hf2) = one_hot_pair(rows_of(first), 16, [rows_of(v_low), rows_of(v_high_first)])
    low_s, (hs1, hs2) = one_hot_pair(rows_of(target), 16, [rows_of(v_low), rows_of(v_high)])
    low = jnp.concatenate([low_f, low_s], 1)
    high = jnp.concatenate([jnp.concatenate([hf1, hs1], 1), jnp.concatenate([hf2, hs2], 1)], 0)
    summed = contract(high, low)
    code = (summed[0:16] + 128.0 * summed[16:32]).astype(I32)
    code_rows = rows_of(code)
    owner_ghost = 1024 + 128 * (sub ^ 1) + 64 + lane
    o_low = ((owner_ghost + 1) & 127).astype(F32)
    o_high = ((owner_ghost + 1) >> 7).astype(F32)
    low_l, (hl1, hl2) = one_hot_pair(rows_of(listed, 6), 16, [rows_of(o_low, 6), rows_of(o_high, 6)])
    linked = contract(jnp.concatenate([hl1, hl2], 0), low_l)
    link_rows = rows_of((linked[0:16] + 128.0 * linked[16:32]).astype(I32))

    at_first, at_second = Index(first), Index(second)
    own1 = jnp.where(joins, slot + 1 + 4096, 0)
    own2 = jnp.where(joins, slot + 1, 0)

    def other(at, mine):
        left = at.look(code_rows) - mine
        via_link = at.look(link_rows)
        number = jnp.where(left > 0, (left & 4095) - 1, via_link - 1)
        sign = jnp.where(left >= 4096, 1.0, -1.0)
        return left, number, sign

    left1, n1, sign1 = other(at_first, own1)
    left2, n2, sign2 = other(at_second, own2)
    n2 = jnp.where(remote, ghost, n2)
    at_n1, at_n2 = Index(n1), Index(n2)
    turn1 = jnp.where(jnp.logical_and(n1 < 1024, sign1 > 0), n1 + 4096, n1)
    turn2 = jnp.where(jnp.logical_and(n2 < 1024, sign2 > 0), n2 + 4096, n2)
    sign1 = jnp.where(n1 >= 1024, 1.0, sign1)
    sign2 = jnp.where(n2 >= 1024, 1.0, sign2)

    face_code = jnp.where(lane < 64, at_list.look(code_rows), code[8:16])
    face_code = jnp.where(sub < 6, face_code, 0)
    face = (face_code & 4095) - 1
    turn1_rows, turn2_rows = rows_of(turn1), rows_of(turn2)
    at_level, ends = [], []
    leaves = jnp.zeros((8, 128), I32)
    current, came_first = face, face_code >= 4096
    for k in range(1, SECOND + 1):
        at = Index(current)
        at_level.append(at)
        ends.append(came_first)
        follow = jnp.where(came_first, at.look(turn2_rows), at.look(turn1_rows))
        follow = jnp.where(current >= 0, follow, -1)
        outside = jnp.logical_and(follow >= 1024, follow < 4096)
        leaves = jnp.where(outside, 1024 * k + follow - 1024, leaves)
        current = jnp.where(jnp.logical_or(outside, follow < 0), -1, follow & 4095)
        came_first = follow >= 4096
    packed = [jnp.where(lane < 64, fields[f], pltpu.roll(fields[f + 4], 64, axis=1)) for f in range(3)] + [fields[3]]
    face_rest = at_level[0].look(rows_of(rest))
    far_atom = jnp.where(ends[0], at_level[0].look(rows_of(second)), at_level[0].look(rows_of(first)))
    at_far = Index(jnp.where(face_rest > 0, far_atom, -1))
    far_fields = [at_far.look(field) for field in own_rows] + [face_rest, leaves.astype(F32)]
    pl.semaphore_wait(barrier, len(offsets(SECOND)))
    atoms = Exchange(0, [[field] for field in packed + far_fields])
    pointers = Exchange(1, [[leaves.astype(F32)]])

    def at_faces(field, depth=1):
        rows = rows_of(field)
        return [at.look(rows) for at in at_level[:depth]]

    def across(value):
        value = pltpu.roll(value, 64, axis=1)
        return jnp.where((sub & 1) == 0, pltpu.roll(value, 7, axis=0), pltpu.roll(value, 1, axis=0))

    from_first = [at_first.look(field) for field in own_rows]
    from_second = [at_second.look(field) for field in own_rows]
    head1 = jnp.logical_and(joins, jnp.logical_or(left1 <= 0, slot < n1))
    head2 = jnp.logical_and(jnp.logical_and(joins, jnp.logical_not(remote)), jnp.logical_or(left2 <= 0, slot < n2))
    head_values = []
    for head, flag in ((head1, 32.0), (head2, 0.0)):
        head_values.append((jnp.where(head, v_low, 0.0), jnp.where(head, v_high + flag, 0.0)))

    def high_of(idx_rows, value_rows):
        parts = []
        for row, value in zip(idx_rows, value_rows):
            hit = jnp.broadcast_to(row >> 7, (8, 128)) == sub
            parts.append(jnp.where(hit, jnp.broadcast_to(value, (8, 128)), 0.0).astype(jnp.bfloat16))
        return jnp.concatenate(parts, 1)

    heads = [
        jnp.concatenate([high_of(rows_of(first), rows_of(head_values[0][k])), high_of(rows_of(target), rows_of(head_values[1][k]))], 1)
        for k in range(2)
    ]
    headed = contract(jnp.concatenate(heads, 0), low)
    head_code = (headed[0:8] + 128.0 * headed[8:16]).astype(I32)

    has_head = head_code > 0
    head_first = head_code >= 4096
    head_slot = (head_code & 4095) - 1
    link = jnp.concatenate(link_rows, 0) - 1
    at_head = Index(head_slot)
    next1 = at_head.look(rows_of(n1))
    next2 = at_head.look(rows_of(n2))
    turn = jnp.where(head_first, 1.0, -1.0)
    tail_slot = jnp.where(has_head, jnp.where(head_first, next1, next2), link)
    at_tail = Index(tail_slot)
    tail_sign = jnp.where(
        head_first, at_head.look(rows_of(sign1)), at_head.look(rows_of(sign2))
    )
    crossed = [across(fields[f]) for f in range(7)]

    atoms.wait()
    at_ghost = [Index(jnp.where(remote, ghost + half, -1)) for half in (0, 64)]
    from_second = [at_ghost[f // 4].look(atoms.faces(f % 4), 8, from_second[f]) for f in range(7)]
    span = [from_first[f] - from_second[f] for f in range(6)]
    mass1, mass2 = from_first[6], from_second[6]
    scale = jnp.where(alive, 1.0, 0.0) / jnp.sqrt(mass1 + mass2)
    inverse = 1.0 / jnp.sqrt(span[0] * span[0] + span[1] * span[1] + span[2] * span[2] + 0.25)
    unit = [span[n] * inverse for n in range(3)]
    arm = [scale * unit[n] for n in range(3)]
    pull = span[3:6]
    x = scale * (unit[0] * pull[0] + unit[1] * pull[1] + unit[2] * pull[2] - rest)

    def dot3(a, b):
        return a[0] * b[0] + a[1] * b[1] + a[2] * b[2]

    mass12 = mass1 + mass2
    diag = 1.0 - dot3(arm, arm) * mass12
    arm_rows = [rows_of(arm[n]) for n in range(3)]
    via1 = [sign1 * at_n1.look(arm_rows[n]) for n in range(3)]
    via2 = [sign2 * at_n2.look(arm_rows[n]) for n in range(3)]

    def near(field):
        rows = rows_of(field)
        return at_n1.look(rows), at_n2.look(rows)

    x1, x2 = near(x)
    diag_levels = at_faces(diag, SECOND - 1)

    here = (0, 0, 0)
    arrived = [atoms.arrived(here, 1, f) for f in range(4)]
    near_atom = [
        jnp.where(lane < 64, arrived[f] if f < 4 else pltpu.roll(arrived[f - 4], 64, axis=1), crossed[f]) for f in range(7)
    ]
    far_atom = [atoms.arrived(here, 1, 4 + f) for f in range(8)]
    leave = atoms.arrived(here, 1, 12).astype(I32)
    leave_lane = leave & 127
    leave_row = jnp.where(leave_lane < 64, leave >> 7, -1)
    seen = {v: [atoms.arrived(v, 1, f) for f in range(4)] for v in offsets(1)}
    for f in range(4):
        slot_ref = fresh("pile", pile_ref)
        for i in range(6):
            slot_ref[8 * i : 8 * i + 8, :] = seen[moved_by(here, i)][f]
        for r in range(6):
            table = slot_ref[pl.ds(r, 8, stride=8), :]
            for half in range(2):
                if f + 4 * half < 7:
                    picked = jnp.take_along_axis(table, (leave_lane + 64 * half) & 127, axis=1)
                    far_atom[f + 4 * half] = jnp.where(leave_row == 8 + r, picked, far_atom[f + 4 * half])
    ghost_rest = far_atom[7]
    there = ghost_rest > 0
    ghost_span = [near_atom[f] - far_atom[f] for f in range(6)]
    ghost_scale = jnp.where(there, 1.0, 0.0) / jnp.sqrt(jnp.where(there, near_atom[6] + far_atom[6], 1.0))
    ghost_unit = [ghost_span[n] / jnp.sqrt(dot3(ghost_span[:3], ghost_span[:3]) + 0.25) for n in range(3)]
    x_ghost = ghost_scale * (dot3(ghost_unit, ghost_span[3:]) - ghost_rest)
    arm_ghosts = [rows_of(ghost_scale * ghost_unit[n], 6) for n in range(3)] + [rows_of(x_ghost, 6)]
    via1 = [mass1 * at_n1.look(arm_ghosts[n], 8, via1[n]) for n in range(3)]
    via2 = [-mass2 * at_n2.look(arm_ghosts[n], 8, via2[n]) for n in range(3)]
    e1 = -dot3(arm, via1)
    e2 = -dot3(arm, via2)
    x1 = at_n1.look(arm_ghosts[3], 8, x1)
    x2 = at_n2.look(arm_ghosts[3], 8, x2)
    e1_rows, e2_rows = rows_of(e1), rows_of(e2)
    onward = [jnp.where(end, at.look(e2_rows), at.look(e1_rows)) for at, end in zip(at_level[: SECOND - 1], ends)]
    inward = across(jnp.where(ends[0], at_level[0].look(e1_rows), at_level[0].look(e2_rows)))

    def step(x, x1, x2, ghosts, diag_ghosts, link_ghosts):
        rows = rows_of(ghosts[0], 6)
        x1 = at_n1.look(rows, 8, x1)
        x2 = at_n2.look(rows, 8, x2)
        chain = [across(at_faces(x)[0]) if len(ghosts) > 1 else None] + ghosts
        ghosts = [
            diag_ghosts[k - 1] * chain[k] + link_ghosts[k - 1] * chain[k - 1] + link_ghosts[k] * chain[k + 1]
            for k in range(1, len(chain) - 1)
        ]
        return diag * x + e1 * x1 + e2 * x2, ghosts

    y = x
    y_ghost = x_ghost
    x, _ = step(x, x1, x2, [y_ghost], None, None)
    moving = Exchange(2, [at_faces(x, FIRST), diag_levels[: FIRST - 1], onward[: FIRST - 1]])
    x1, x2 = near(x)
    pointers.wait()
    exits = {v: Index(pointers.arrived(v, 1, 0).astype(I32)) for v in [(0, 0, 0)] + offsets(SECOND - 2)}
    moving.wait()
    diag_ghosts = moving.ghosts(1, FIRST - 1, exits)
    link_ghosts = [inward] + moving.ghosts(2, FIRST - 1, exits)
    ghosts = moving.ghosts(0, FIRST, exits)
    for n in range(ORDER):
        y = y + x
        y_ghost = y_ghost + ghosts[0]
        if n == ORDER - 1:
            break
        x, ghosts = step(x, x1, x2, ghosts, diag_ghosts, link_ghosts)
        x1, x2 = near(x)

    at_exit = Index(leaves)

    def resolved(value, ghost_levels):
        for t in range(1, SECOND - 1):
            value = at_exit.look(rows_of(ghost_levels[SECOND - 2 - t], 6), 8 * t, value)
        return value

    relayed = [[resolved(diag_levels[-1], diag_ghosts)], [resolved(onward[-1], link_ghosts[1:])]]
    y1, y2 = near(y)
    rows = rows_of(y_ghost, 6)
    y1 = at_n1.look(rows, 8, y1)
    y2 = at_n2.look(rows, 8, y2)
    stretch = [pull[n] - (mass12 * arm[n] * y + via1[n] * y1 + via2[n] * y2) for n in range(3)]
    square = rest * rest
    goal = jnp.sqrt(jnp.maximum(2.0 * square - dot3(stretch, stretch), 0.25 * square))
    x = scale * (rest - goal)
    moving = Exchange(3, [at_faces(x, SECOND)] + relayed)

    x1, x2 = near(x)
    arm_head = [turn * at_head.look(arm_rows[n]) for n in range(3)]
    arm_tail = [at_tail.look(arm_ghosts[n], 8, tail_sign * at_tail.look(arm_rows[n])) for n in range(3)]
    moving.wait()
    diag_ghosts = diag_ghosts + [moving.arrived(here, 1, 1)]
    link_ghosts = link_ghosts + [moving.arrived(here, 1, 2)]
    ghosts = moving.ghosts(0, SECOND, exits)
    z, z_ghost = y, y_ghost
    for n in range(ORDER + 1):
        z = z + x
        z_ghost = z_ghost + ghosts[0]
        if n == ORDER:
            break
        x, ghosts = step(x, x1, x2, ghosts, diag_ghosts, link_ghosts)
        x1, x2 = near(x)
    mult_ref[...] = z

    z_rows = rows_of(z)
    z_head = at_head.look(z_rows)
    z_tail = at_tail.look(z_rows)
    z_tail = at_tail.look(rows_of(z_ghost, 6), 8, z_tail)
    for n in range(3):
        moved = -mass * (arm_head[n] * z_head + arm_tail[n] * z_tail)
        for j in range(8):
            disp_ref[n : n + 1, 128 * j : 128 * j + 128] = moved[j : j + 1, :]


def per_device(old_pos, new_pos, inv_mass, rest_length, bond_pairs, live, send_index):
    vmem = pl.BlockSpec(memory_space=pltpu.VMEM)
    disp, mult = pl.pallas_call(
        kernel,
        out_shape=(pltpu.VMEM((3, 1024), F32), pltpu.VMEM((8, 128), F32)),
        in_specs=[pl.BlockSpec(memory_space=pl.ANY)] * 7,
        out_specs=(vmem, vmem),
        scratch_shapes=[pltpu.VMEM((512, 8, 128), F32), pltpu.VMEM((8, 128), I32), pltpu.VMEM((192, 64, 128), F32)]
        + [pltpu.VMEM(shape, kind) for shape, kind in GIVEN]
        + [pltpu.SemaphoreType.DMA((7,))]
        + [shape for plan in plans() for shape in plan.shapes()],
        compiler_params=pltpu.CompilerParams(collective_id=0, has_side_effects=True),
        name="plincs",
    )(
        old_pos,
        new_pos,
        inv_mass.reshape(8, 128),
        rest_length.reshape(8, 128),
        bond_pairs,
        live.reshape(8, 128),
        send_index,
    )
    return disp, mult.reshape(1024)


def solution(mesh):
    in_specs = (
        P(None, ("gx", "gy", "gz")),
        P(None, ("gx", "gy", "gz")),
        P(("gx", "gy", "gz")),
        P(("gx", "gy", "gz")),
        P(None, ("gx", "gy", "gz")),
        P(("gx", "gy", "gz")),
        P(("gx", "gy", "gz"), None),
    )
    out_specs = (P(None, ("gx", "gy", "gz")), P(("gx", "gy", "gz")))
    return jax.shard_map(
        per_device, mesh=mesh, in_specs=in_specs, out_specs=out_specs, check_vma=False
    )
```

```python
import jax
import jax.numpy as jnp
from jax import lax
from jax.experimental import pallas as pl
from jax.experimental.pallas import tpu as pltpu
from jax.sharding import PartitionSpec as P

MESH = pl.DeviceIdType.MESH
ORDER = 4
W = 48
F32 = jnp.float32
I32 = jnp.int32
GIVEN = (((3, 1024), F32), ((3, 1024), F32), ((8, 128), F32), ((8, 128), F32), ((2, 1024), I32), ((8, 128), I32), ((6, W), I32))
FIRST, SECOND = 4, 5
LIST_ROW = (0, 1, 4, 5, 2, 3)
STEPS = ((1, 0, 0), (1, 0, 0), (0, 0, -1), (0, 0, 1), (0, 1, 0), (0, 1, 0))


def moved_by(o, i, turn=1):
    s = STEPS[i]
    return ((o[0] + s[0]) % 2, (o[1] + s[1]) % 2, o[2] + turn * s[2])


def dist(o):
    return o[0] + o[1] + abs(o[2])


def offsets(depth):
    every = [(x, y, z) for x in range(2) for y in range(2) for z in range(-depth, depth + 1)]
    return [o for o in every if 0 < dist(o) <= depth]


class Plan:
    def __init__(self, *fields):
        self.messages, self.place, self.rows = [], {}, 0
        for o in sorted(offsets(max(depth for depth, _ in fields)), key=lambda o: -dist(o)):
            start = self.rows
            for f, (depth, levels) in enumerate(fields):
                for i in range(6):
                    for k in range(1, min(levels, depth - dist(moved_by(o, i, -1))) + 1):
                        self.place[o, k, i, f] = self.rows
                        self.rows += 1
            self.messages.append((o, start, self.rows - start))

    def shapes(self):
        rows = pltpu.VMEM((self.rows, 1, 128), F32)
        sems = pltpu.SemaphoreType.DMA((len(self.messages),))
        return [rows, rows, sems, sems]


def plans():
    return [
        Plan(*[(2, 1)] * 4 + [(1, 1)] * 9),
        Plan((SECOND - 1, 1)),
        Plan((FIRST, FIRST), (FIRST - 1, FIRST - 1), (FIRST - 1, FIRST - 1)),
        Plan((SECOND, SECOND), (1, 1), (1, 1)),
    ]


def lane_pick(row, lo):
    return jnp.take_along_axis(jnp.broadcast_to(row, (8, 128)), lo, axis=1)


class Index:
    def __init__(self, idx):
        self.lo = idx & 127
        self.hi = idx >> 7

    def look(self, rows, base=0, start=None):
        out = jnp.zeros((8, 128), rows[0].dtype) if start is None else start
        for j, row in enumerate(rows):
            out = jnp.where(self.hi == base + j, lane_pick(row, self.lo), out)
        return out


def rows_of(tile, count=8):
    return [tile[j : j + 1, :] for j in range(count)]


def one_hot_pair(idx_rows, hi_count, values):
    low, high = [], [[] for _ in values]
    for j, row in enumerate(idx_rows):
        lo = jnp.broadcast_to(row & 127, (128, 128))
        low.append(jnp.where(lo == lax.broadcasted_iota(I32, (128, 128), 0), 1.0, 0.0).astype(jnp.bfloat16))
        hit = jnp.broadcast_to(row >> 7, (hi_count, 128)) == lax.broadcasted_iota(I32, (hi_count, 128), 0)
        for k, value in enumerate(values):
            picked = jnp.where(hit, jnp.broadcast_to(value[j], (hi_count, 128)), 0.0)
            high[k].append(picked.astype(jnp.bfloat16))
    return jnp.concatenate(low, 1), [jnp.concatenate(h, 1) for h in high]


def contract(a, b):
    return lax.dot_general(a, b, (((1,), (1,)), ((), ())), preferred_element_type=F32)


def kernel(*refs):
    given, (disp_ref, mult_ref, tile_ref, list_ref, pile_ref), bufs = refs[:7], refs[7:12], refs[12:]
    taken, take_sem, bufs = bufs[:7], bufs[7], bufs[8:]
    ix, iy, iz = lax.axis_index("gx"), lax.axis_index("gy"), lax.axis_index("gz")
    nz = lax.axis_size("gz")

    def peer(o):
        device = {}
        if o[0]:
            device["gx"] = 1 - ix
        if o[1]:
            device["gy"] = 1 - iy
        if o[2]:
            device["gz"] = lax.rem(iz + nz - o[2], nz)
        return device

    takes = [pltpu.make_async_copy(given[n], taken[n], take_sem.at[n]) for n in range(7)]
    for n in (6, 0, 1, 2, 4, 5, 3):
        takes[n].start()
    barrier = pltpu.get_barrier_semaphore()
    for o in offsets(SECOND):
        pl.semaphore_signal(barrier, inc=1, device_id=peer(o), device_id_type=MESH)

    old_ref, new_ref, mass_ref, rest_ref, pair_ref, live_ref, send_ref = taken

    todo = plans()

    count = {"tile": 6, "pile": 0}

    def fresh(name, ref, low=0):
        n = count[name]
        count[name] = n + 1 if n + 1 < ref.shape[0] else low
        return ref.at[n]

    class Exchange:
        def __init__(self, number, levels):
            self.plan = plan = todo[number]
            self.own = levels
            out, self.box, ssem, rsem = bufs[4 * number : 4 * number + 4]
            self.copies = []
            for n, (o, start, count) in enumerate(plan.messages):
                for (offset, k, i, f), row in plan.place.items():
                    if offset == o:
                        out[row] = levels[f][k - 1][i : i + 1, :]
            for n, (o, start, count) in enumerate(plan.messages):
                copy = pltpu.make_async_remote_copy(
                    src_ref=out.at[pl.ds(start, count)],
                    dst_ref=self.box.at[pl.ds(start, count)],
                    send_sem=ssem.at[n],
                    recv_sem=rsem.at[n],
                    device_id=peer(o),
                    device_id_type=MESH,
                )
                copy.start()
                self.copies.append(copy)

        def wait(self):
            for copy in self.copies:
                copy.wait()

        def row(self, o, k, i, f):
            if dist(o) == 0:
                return self.own[f][k - 1][i : i + 1, :]
            return self.box[self.plan.place[o, k, i, f]]

        def faces(self, f):
            return [self.row(moved_by((0, 0, 0), i), 1, i, f) for i in range(6)]

        def arrived(self, v, k, f):
            out = jnp.broadcast_to(self.row(moved_by(v, 0), k, 0, f), (8, 128))
            for i in range(1, 6):
                out = jnp.where(sub == i, self.row(moved_by(v, i), k, i, f), out)
            return out

        def ghosts(self, f, depth, exits):
            here = [(0, 0, 0)] + offsets(depth - 1)
            values = {v: [self.arrived(v, k, f) for k in range(1, depth - dist(v) + 1)] for v in here}
            for j in range(1, depth):
                for v in here:
                    if dist(v) > depth - j - 1:
                        continue
                    slot_ref = fresh("pile", pile_ref)
                    for i in range(6):
                        slot_ref[8 * i : 8 * i + 8, :] = values[moved_by(v, i)][j - 1]
                    at = exits[v]
                    for r in range(6):
                        picked = jnp.take_along_axis(slot_ref[pl.ds(r, 8, stride=8), :], at.lo, axis=1)
                        for k in range(j + 1, depth - dist(v) + 1):
                            values[v][k - 1] = jnp.where(at.hi == 8 * (k - j) + r, picked, values[v][k - 1])
            return values[(0, 0, 0)]

    def tile(n, ref, row):
        for j in range(8):
            tile_ref[n, j : j + 1, :] = ref[row : row + 1, 128 * j : 128 * j + 128]
        return tile_ref[n]

    lane = lax.broadcasted_iota(I32, (8, 128), 1)
    sub = lax.broadcasted_iota(I32, (8, 128), 0)
    slot = sub * 128 + lane

    for take in takes:
        take.wait()
    list_ref[...] = jnp.full((8, 128), -1, I32)
    for b in range(6):
        list_ref[LIST_ROW[b] : LIST_ROW[b] + 1, 0:W] = send_ref[b : b + 1, :]
    listed = list_ref[...]
    at_list = Index(listed)
    own = [tile(n, old_ref, n) for n in range(3)] + [tile(3 + n, new_ref, n) for n in range(3)] + [mass_ref[...]]
    own_rows = [rows_of(field) for field in own]
    fields = [at_list.look(field) for field in own_rows]

    mass = own[6]
    rest = rest_ref[...]
    alive = live_ref[...] != 0
    pair_rows = [[pair_ref[r : r + 1, 128 * j : 128 * j + 128] for j in range(8)] for r in range(2)]
    for r in range(2):
        for j in range(8):
            list_ref[j : j + 1, :] = pair_rows[r][j]
        if r == 0:
            first = list_ref[...]
        else:
            second = list_ref[...]
    off = second - 1024
    block = jnp.zeros((8, 128), I32)
    for t in range(1, 6):
        block = block + jnp.where(off >= W * t, 1, 0)
    remote = off >= 0
    lane_in = off - W * block
    block = block + jnp.where(block >= 4, -2, jnp.where(block >= 2, 2, 0))
    ghost = 1024 + 128 * block + lane_in
    target = jnp.where(remote, 1024 + 128 * (block ^ 1) + 64 + lane_in, second)
    joins = jnp.logical_and(alive, first != second)
    label = jnp.where(joins, slot + 1, 0)
    v_low = (label & 127).astype(F32)
    v_high = (label >> 7).astype(F32)
    v_high_first = v_high + jnp.where(joins, 32.0, 0.0)
    low_f, (hf1, hf2) = one_hot_pair(rows_of(first), 16, [rows_of(v_low), rows_of(v_high_first)])
    low_s, (hs1, hs2) = one_hot_pair(rows_of(target), 16, [rows_of(v_low), rows_of(v_high)])
    low = jnp.concatenate([low_f, low_s], 1)
    high = jnp.concatenate([jnp.concatenate([hf1, hs1], 1), jnp.concatenate([hf2, hs2], 1)], 0)
    summed = contract(high, low)
    code = (summed[0:16] + 128.0 * summed[16:32]).astype(I32)
    code_rows = rows_of(code)
    owner_ghost = 1024 + 128 * (sub ^ 1) + 64 + lane
    o_low = ((owner_ghost + 1) & 127).astype(F32)
    o_high = ((owner_ghost + 1) >> 7).astype(F32)
    low_l, (hl1, hl2) = one_hot_pair(rows_of(listed, 6), 16, [rows_of(o_low, 6), rows_of(o_high, 6)])
    linked = contract(jnp.concatenate([hl1, hl2], 0), low_l)
    link_rows = rows_of((linked[0:16] + 128.0 * linked[16:32]).astype(I32))

    at_first, at_second = Index(first), Index(second)
    own1 = jnp.where(joins, slot + 1 + 4096, 0)
    own2 = jnp.where(joins, slot + 1, 0)

    def other(at, mine):
        left = at.look(code_rows) - mine
        via_link = at.look(link_rows)
        number = jnp.where(left > 0, (left & 4095) - 1, via_link - 1)
        sign = jnp.where(left >= 4096, 1.0, -1.0)
        return left, number, sign

    left1, n1, sign1 = other(at_first, own1)
    left2, n2, sign2 = other(at_second, own2)
    n2 = jnp.where(remote, ghost, n2)
    at_n1, at_n2 = Index(n1), Index(n2)
    turn1 = jnp.where(jnp.logical_and(n1 < 1024, sign1 > 0), n1 + 4096, n1)
    turn2 = jnp.where(jnp.logical_and(n2 < 1024, sign2 > 0), n2 + 4096, n2)
    sign1 = jnp.where(n1 >= 1024, 1.0, sign1)
    sign2 = jnp.where(n2 >= 1024, 1.0, sign2)

    face_code = jnp.where(lane < 64, at_list.look(code_rows), code[8:16])
    face_code = jnp.where(sub < 6, face_code, 0)
    face = (face_code & 4095) - 1
    turn1_rows, turn2_rows = rows_of(turn1), rows_of(turn2)
    at_level, ends = [], []
    leaves = jnp.zeros((8, 128), I32)
    current, came_first = face, face_code >= 4096
    for k in range(1, SECOND + 1):
        at = Index(current)
        at_level.append(at)
        ends.append(came_first)
        follow = jnp.where(came_first, at.look(turn2_rows), at.look(turn1_rows))
        follow = jnp.where(current >= 0, follow, -1)
        outside = jnp.logical_and(follow >= 1024, follow < 4096)
        leaves = jnp.where(outside, 1024 * k + follow - 1024, leaves)
        current = jnp.where(jnp.logical_or(outside, follow < 0), -1, follow & 4095)
        came_first = follow >= 4096
    packed = [jnp.where(lane < 64, fields[f], pltpu.roll(fields[f + 4], 64, axis=1)) for f in range(3)] + [fields[3]]
    face_rest = at_level[0].look(rows_of(rest))
    far_atom = jnp.where(ends[0], at_level[0].look(rows_of(second)), at_level[0].look(rows_of(first)))
    at_far = Index(jnp.where(face_rest > 0, far_atom, -1))
    far_fields = [at_far.look(field) for field in own_rows] + [face_rest, leaves.astype(F32)]
    pl.semaphore_wait(barrier, len(offsets(SECOND)))
    atoms = Exchange(0, [[field] for field in packed + far_fields])
    pointers = Exchange(1, [[leaves.astype(F32)]])

    def at_faces(field, depth=1):
        rows = rows_of(field)
        return [at.look(rows) for at in at_level[:depth]]

    def across(value):
        value = pltpu.roll(value, 64, axis=1)
        return jnp.where((sub & 1) == 0, pltpu.roll(value, 7, axis=0), pltpu.roll(value, 1, axis=0))

    from_first = [at_first.look(field) for field in own_rows]
    from_second = [at_second.look(field) for field in own_rows]
    head1 = jnp.logical_and(joins, jnp.logical_or(left1 <= 0, slot < n1))
    head2 = jnp.logical_and(jnp.logical_and(joins, jnp.logical_not(remote)), jnp.logical_or(left2 <= 0, slot < n2))
    head_values = []
    for head, flag in ((head1, 32.0), (head2, 0.0)):
        head_values.append((jnp.where(head, v_low, 0.0), jnp.where(head, v_high + flag, 0.0)))

    def high_of(idx_rows, value_rows):
        parts = []
        for row, value in zip(idx_rows, value_rows):
            hit = jnp.broadcast_to(row >> 7, (8, 128)) == sub
            parts.append(jnp.where(hit, jnp.broadcast_to(value, (8, 128)), 0.0).astype(jnp.bfloat16))
        return jnp.concatenate(parts, 1)

    heads = [
        jnp.concatenate([high_of(rows_of(first), rows_of(head_values[0][k])), high_of(rows_of(target), rows_of(head_values[1][k]))], 1)
        for k in range(2)
    ]
    headed = contract(jnp.concatenate(heads, 0), low)
    head_code = (headed[0:8] + 128.0 * headed[8:16]).astype(I32)

    has_head = head_code > 0
    head_first = head_code >= 4096
    head_slot = (head_code & 4095) - 1
    link = jnp.concatenate(link_rows, 0) - 1
    at_head = Index(head_slot)
    next1 = at_head.look(rows_of(n1))
    next2 = at_head.look(rows_of(n2))
    turn = jnp.where(head_first, 1.0, -1.0)
    tail_slot = jnp.where(has_head, jnp.where(head_first, next1, next2), link)
    at_tail = Index(tail_slot)
    tail_sign = jnp.where(
        head_first, at_head.look(rows_of(sign1)), at_head.look(rows_of(sign2))
    )
    crossed = [across(fields[f]) for f in range(7)]

    atoms.wait()
    at_ghost = [Index(jnp.where(remote, ghost + half, -1)) for half in (0, 64)]
    from_second = [at_ghost[f // 4].look(atoms.faces(f % 4), 8, from_second[f]) for f in range(7)]
    span = [from_first[f] - from_second[f] for f in range(6)]
    mass1, mass2 = from_first[6], from_second[6]
    scale = jnp.where(alive, 1.0, 0.0) / jnp.sqrt(mass1 + mass2)
    inverse = 1.0 / jnp.sqrt(span[0] * span[0] + span[1] * span[1] + span[2] * span[2] + 0.25)
    unit = [span[n] * inverse for n in range(3)]
    arm = [scale * unit[n] for n in range(3)]
    pull = span[3:6]
    x = scale * (unit[0] * pull[0] + unit[1] * pull[1] + unit[2] * pull[2] - rest)

    def dot3(a, b):
        return a[0] * b[0] + a[1] * b[1] + a[2] * b[2]

    mass12 = mass1 + mass2
    diag = 1.0 - dot3(arm, arm) * mass12
    arm_rows = [rows_of(arm[n]) for n in range(3)]
    via1 = [sign1 * at_n1.look(arm_rows[n]) for n in range(3)]
    via2 = [sign2 * at_n2.look(arm_rows[n]) for n in range(3)]

    def near(field):
        rows = rows_of(field)
        return at_n1.look(rows), at_n2.look(rows)

    x1, x2 = near(x)
    diag_levels = at_faces(diag, SECOND - 1)

    here = (0, 0, 0)
    arrived = [atoms.arrived(here, 1, f) for f in range(4)]
    near_atom = [
        jnp.where(lane < 64, arrived[f] if f < 4 else pltpu.roll(arrived[f - 4], 64, axis=1), crossed[f]) for f in range(7)
    ]
    far_atom = [atoms.arrived(here, 1, 4 + f) for f in range(8)]
    leave = atoms.arrived(here, 1, 12).astype(I32)
    leave_lane = leave & 127
    leave_row = jnp.where(leave_lane < 64, leave >> 7, -1)
    seen = {v: [atoms.arrived(v, 1, f) for f in range(4)] for v in offsets(1)}
    for f in range(4):
        slot_ref = fresh("pile", pile_ref)
        for i in range(6):
            slot_ref[8 * i : 8 * i + 8, :] = seen[moved_by(here, i)][f]
        for r in range(6):
            table = slot_ref[pl.ds(r, 8, stride=8), :]
            for half in range(2):
                if f + 4 * half < 7:
                    picked = jnp.take_along_axis(table, (leave_lane + 64 * half) & 127, axis=1)
                    far_atom[f + 4 * half] = jnp.where(leave_row == 8 + r, picked, far_atom[f + 4 * half])
    ghost_rest = far_atom[7]
    there = ghost_rest > 0
    ghost_span = [near_atom[f] - far_atom[f] for f in range(6)]
    ghost_scale = jnp.where(there, 1.0, 0.0) / jnp.sqrt(jnp.where(there, near_atom[6] + far_atom[6], 1.0))
    ghost_unit = [ghost_span[n] / jnp.sqrt(dot3(ghost_span[:3], ghost_span[:3]) + 0.25) for n in range(3)]
    x_ghost = ghost_scale * (dot3(ghost_unit, ghost_span[3:]) - ghost_rest)
    arm_ghosts = [rows_of(ghost_scale * ghost_unit[n], 6) for n in range(3)] + [rows_of(x_ghost, 6)]
    via1 = [mass1 * at_n1.look(arm_ghosts[n], 8, via1[n]) for n in range(3)]
    via2 = [-mass2 * at_n2.look(arm_ghosts[n], 8, via2[n]) for n in range(3)]
    e1 = -dot3(arm, via1)
    e2 = -dot3(arm, via2)
    x1 = at_n1.look(arm_ghosts[3], 8, x1)
    x2 = at_n2.look(arm_ghosts[3], 8, x2)
    e1_rows, e2_rows = rows_of(e1), rows_of(e2)
    onward = [jnp.where(end, at.look(e2_rows), at.look(e1_rows)) for at, end in zip(at_level[: SECOND - 1], ends)]
    inward = across(jnp.where(ends[0], at_level[0].look(e1_rows), at_level[0].look(e2_rows)))

    at_cross = Index(across(face))

    def step(x, x1, x2, ghosts, diag_ghosts, link_ghosts):
        rows = rows_of(ghosts[0], 6)
        x1 = at_n1.look(rows, 8, x1)
        x2 = at_n2.look(rows, 8, x2)
        chain = [at_cross.look(rows_of(x)) if len(ghosts) > 1 else None] + ghosts
        ghosts = [
            diag_ghosts[k - 1] * chain[k] + link_ghosts[k - 1] * chain[k - 1] + link_ghosts[k] * chain[k + 1]
            for k in range(1, len(chain) - 1)
        ]
        return diag * x + e1 * x1 + e2 * x2, ghosts

    y = x
    y_ghost = x_ghost
    x, _ = step(x, x1, x2, [y_ghost], None, None)
    moving = Exchange(2, [at_faces(x, FIRST), diag_levels[: FIRST - 1], onward[: FIRST - 1]])
    x1, x2 = near(x)
    pointers.wait()
    exits = {v: Index(pointers.arrived(v, 1, 0).astype(I32)) for v in [(0, 0, 0)] + offsets(SECOND - 2)}
    moving.wait()
    diag_ghosts = moving.ghosts(1, FIRST - 1, exits)
    link_ghosts = [inward] + moving.ghosts(2, FIRST - 1, exits)
    ghosts = moving.ghosts(0, FIRST, exits)
    for n in range(ORDER):
        y = y + x
        y_ghost = y_ghost + ghosts[0]
        if n == ORDER - 1:
            break
        x, ghosts = step(x, x1, x2, ghosts, diag_ghosts, link_ghosts)
        x1, x2 = near(x)

    at_exit = Index(leaves)

    def resolved(value, ghost_levels):
        for t in range(1, SECOND - 1):
            value = at_exit.look(rows_of(ghost_levels[SECOND - 2 - t], 6), 8 * t, value)
        return value

    relayed = [[resolved(diag_levels[-1], diag_ghosts)], [resolved(onward[-1], link_ghosts[1:])]]
    y1, y2 = near(y)
    rows = rows_of(y_ghost, 6)
    y1 = at_n1.look(rows, 8, y1)
    y2 = at_n2.look(rows, 8, y2)
    stretch = [pull[n] - (mass12 * arm[n] * y + via1[n] * y1 + via2[n] * y2) for n in range(3)]
    square = rest * rest
    goal = jnp.sqrt(jnp.maximum(2.0 * square - dot3(stretch, stretch), 0.25 * square))
    x = scale * (rest - goal)
    moving = Exchange(3, [at_faces(x, SECOND)] + relayed)

    x1, x2 = near(x)
    arm_head = [turn * at_head.look(arm_rows[n]) for n in range(3)]
    arm_tail = [at_tail.look(arm_ghosts[n], 8, tail_sign * at_tail.look(arm_rows[n])) for n in range(3)]
    moving.wait()
    diag_ghosts = diag_ghosts + [moving.arrived(here, 1, 1)]
    link_ghosts = link_ghosts + [moving.arrived(here, 1, 2)]
    ghosts = moving.ghosts(0, SECOND, exits)
    z, z_ghost = y, y_ghost
    for n in range(ORDER + 1):
        z = z + x
        z_ghost = z_ghost + ghosts[0]
        if n == ORDER:
            break
        x, ghosts = step(x, x1, x2, ghosts, diag_ghosts, link_ghosts)
        x1, x2 = near(x)
    mult_ref[...] = z

    z_rows = rows_of(z)
    z_head = at_head.look(z_rows)
    z_tail = at_tail.look(z_rows)
    z_tail = at_tail.look(rows_of(z_ghost, 6), 8, z_tail)
    for n in range(3):
        moved = -mass * (arm_head[n] * z_head + arm_tail[n] * z_tail)
        for j in range(8):
            disp_ref[n : n + 1, 128 * j : 128 * j + 128] = moved[j : j + 1, :]


def per_device(old_pos, new_pos, inv_mass, rest_length, bond_pairs, live, send_index):
    vmem = pl.BlockSpec(memory_space=pltpu.VMEM)
    disp, mult = pl.pallas_call(
        kernel,
        out_shape=(pltpu.VMEM((3, 1024), F32), pltpu.VMEM((8, 128), F32)),
        in_specs=[pl.BlockSpec(memory_space=pl.ANY)] * 7,
        out_specs=(vmem, vmem),
        scratch_shapes=[pltpu.VMEM((512, 8, 128), F32), pltpu.VMEM((8, 128), I32), pltpu.VMEM((192, 64, 128), F32)]
        + [pltpu.VMEM(shape, kind) for shape, kind in GIVEN]
        + [pltpu.SemaphoreType.DMA((7,))]
        + [shape for plan in plans() for shape in plan.shapes()],
        compiler_params=pltpu.CompilerParams(collective_id=0, has_side_effects=True),
        name="plincs",
    )(
        old_pos,
        new_pos,
        inv_mass.reshape(8, 128),
        rest_length.reshape(8, 128),
        bond_pairs,
        live.reshape(8, 128),
        send_index,
    )
    return disp, mult.reshape(1024)


def solution(mesh):
    in_specs = (
        P(None, ("gx", "gy", "gz")),
        P(None, ("gx", "gy", "gz")),
        P(("gx", "gy", "gz")),
        P(("gx", "gy", "gz")),
        P(None, ("gx", "gy", "gz")),
        P(("gx", "gy", "gz")),
        P(("gx", "gy", "gz"), None),
    )
    out_specs = (P(None, ("gx", "gy", "gz")), P(("gx", "gy", "gz")))
    return jax.shard_map(
        per_device, mesh=mesh, in_specs=in_specs, out_specs=out_specs, check_vma=False
    )
```
